8 devices in a mesh: dp: 2 (over y, z), tp: 4 (over x, core).
Axes of the slice: x: 2, y: 2, z: 1, core: 2. Of those that a mesh axis runs over, the one named last changes fastest.
Arguments:
- x: bfloat16 [256, 5120], P('dp'), parts along dimension 0
- w_gate: bfloat16 [5120, 17920], P(None, 'tp')
- w_up: bfloat16 [5120, 17920], P(None, 'tp')
- w_down: bfloat16 [17920, 5120], P('tp')
Outputs:
- output: bfloat16 [256, 5120], P('dp'), parts along dimension 0
There are 2 independent parts. The reference program is written for one: setup_inputs(seed, part) draws one part's arguments, and reference() takes and returns one part's arrays. A program takes and returns all parts, laid end to end along the dimension named above; an argument that names none is the same for every part.
All inputs are finite; a program needn't handle non-finite values.
Results may differ from the reference program's by a relative error of at most 0.016.
Values are sent between devices in bfloat16 or wider.
A program may use at most 2 GiB of HBM per device.

```python
import jax
import jax.numpy as jnp

ROWS = 128
D = 5120
FF = 17920


def setup_inputs(seed: int = 0, part: int = 0) -> dict:
    kx, kg, ku, kd = jax.random.split(jax.random.key(seed), 4)
    drawn = {
        "x": jax.random.normal(jax.random.fold_in(kx, part), (ROWS, D), jnp.float32),
        "w_gate": jax.random.normal(kg, (D, FF), jnp.float32) * D**-0.5,
        "w_up": jax.random.normal(ku, (D, FF), jnp.float32) * D**-0.5,
        "w_down": jax.random.normal(kd, (FF, D), jnp.float32) * FF**-0.5,
    }
    return {k: v.astype(jnp.bfloat16) for k, v in drawn.items()}


def reference(x, w_gate, w_up, w_down):
    gate = jnp.dot(x, w_gate, preferred_element_type=jnp.float32)
    up = jnp.dot(x, w_up, preferred_element_type=jnp.float32)
    hidden = (jax.nn.silu(gate) * up).astype(jnp.bfloat16)
    return jnp.dot(hidden, w_down, preferred_element_type=jnp.float32).astype(jnp.bfloat16)
```

```python
import jax
import jax.numpy as jnp
from jax import lax
from jax.experimental import pallas as pl
from jax.experimental.pallas import tpu as pltpu
from jax.sharding import PartitionSpec as P

MESH = pl.DeviceIdType.MESH
ROWS, D, FF = 128, 5120, 4480
U = 2304
SKIP = FF - U
KC = 512
NK = D // KC
NC = 512
NN = D // NC
HC = NC // 2
GS = 5
DS = 5
LAG_Y, LAG_X = 4, 6
F32, BF16 = jnp.float32, jnp.bfloat16


def kernel(x, wg, wu, wd, o, X, acc, h, gu, dn, mine, msend, mrecv, ysend, yrecv, xsend, xrecv,
           xsem, gsem, dsem, in_y, in_x, in_m, out_m, out_y, out_x, out_o):
    d, t = lax.axis_index("dp"), lax.axis_index("tp")
    xi, c = t // 2, t % 2
    mate, ypeer, xpeer = (d, t + 1 - 2 * c), (1 - d, t), (d, (t + 2) % 4)
    unit0 = pl.multiple_of(d * SKIP, 128)

    def remote(src, dst, sems, i, peer):
        return pltpu.make_async_remote_copy(
            src_ref=src, dst_ref=dst, send_sem=sems.at[0, i], recv_sem=sems.at[1, i], device_id=peer, device_id_type=MESH)

    def chunk(i):
        pair = (i - 2) // 2
        j = jnp.where(i < 2, i, jnp.where(i < 8, jnp.where(i % 2 == 0, pair + 2, pair), i - 5))
        relayed = jnp.where(i < 8, jnp.where(i < 2, 0, i % 2), 1)
        return 2 * j + jnp.where(relayed == 1, 1 - xi, xi)

    def x_own(k):
        return pltpu.make_async_copy(x.at[:, pl.ds(k * KC, KC)], X.at[k, pl.ds(0, ROWS)], xsem.at[k])

    def slab(i, which):
        w = (wg, wu)[which]
        rows = pl.ds(pl.multiple_of(chunk(i) * KC, KC), KC)
        s = i % GS
        return pltpu.make_async_copy(w.at[rows, pl.ds(unit0, U)], gu.at[s, which], gsem.at[s, which])

    def down(n, half):
        s = n % DS
        cols = pl.ds(pl.multiple_of(n * NC + jnp.where(half == 0, c, 1 - c) * HC, HC), HC)
        return pltpu.make_async_copy(
            wd.at[pl.ds(unit0, U), cols], dn.at[s, :, pl.ds(half * HC, HC)], dsem.at[s, half])

    def other(k, core):
        return X.at[k, pl.ds(ROWS, ROWS), pl.ds(pl.multiple_of(core * (KC // 2), KC // 2), KC // 2)]

    def mine_x(k):
        return X.at[k, pl.ds(0, ROWS), pl.ds(pl.multiple_of(c * (KC // 2), KC // 2), KC // 2)]

    def send_y(j):
        return remote(mine_x(2 * j + xi), other(2 * j + xi, c), in_y, j, ypeer)

    def relay_x(j):
        return remote(other(2 * j + xi, c), other(2 * j + xi, c), in_x, j, xpeer)

    def got_x(j):
        return remote(other(2 * j + 1 - xi, c), other(2 * j + 1 - xi, c), in_x, j, xpeer)

    def to_mate(j, relayed):
        k = 2 * j + (1 - xi if relayed else xi)
        return remote(other(k, c), other(k, c), in_m, j + 5 * relayed, mate)

    def from_mate(j, relayed):
        k = 2 * j + (1 - xi if relayed else xi)
        return remote(other(k, 1 - c), other(k, 1 - c), in_m, j + 5 * relayed, mate)

    for k in range(NK):
        x_own(k).start()
    for i in range(GS):
        slab(i, 0).start()
        slab(i, 1).start()
    barrier = pltpu.get_barrier_semaphore()
    for peer in (mate, ypeer, xpeer):
        pl.semaphore_signal(barrier, inc=1, device_id=peer, device_id_type=MESH)
    pl.semaphore_wait(barrier, 3)
    for k in range(NK):
        x_own(k).wait()
    for j in range(5):
        send_y(j).start()
    acc[...] = jnp.zeros_like(acc)
    for n in range(DS):
        down(n, 0).start()
        down(n, 1).start()

    def direct(j):
        send_y(j).wait_recv()
        relay_x(j).start()
        to_mate(j, 0).start()

    direct(0)

    @pl.loop(0, NK)
    def _(i):
        @pl.when(i < 4)
        def _():
            direct(i + 1)

        @pl.when(jnp.logical_and(i >= 2, i < 7))
        def _():
            got_x(i - 2).wait_recv()
            to_mate(i - 2, 1).start()

        @pl.when(i < 2)
        def _():
            from_mate(i, 0).wait_recv()

        @pl.when(jnp.logical_and(i >= 2, i < 8))
        def _():
            @pl.when(i % 2 == 0)
            def _():
                from_mate((i - 2) // 2 + 2, 0).wait_recv()

            @pl.when(i % 2 == 1)
            def _():
                from_mate((i - 2) // 2, 1).wait_recv()

        @pl.when(i >= 8)
        def _():
            from_mate(i - 5, 1).wait_recv()

        k = chunk(i)
        s = i % GS
        xk = X[k]
        for which in range(2):
            slab(i, which).wait()
            acc[:, which * U:(which + 1) * U] += jnp.dot(xk, gu[s, which], preferred_element_type=F32)

            @pl.when(i + GS < NK)
            def _():
                slab(i + GS, which).start()

    @pl.loop(0, U // 256)
    def _(b):
        g = acc[:, pl.ds(pl.multiple_of(b * 256, 256), 256)]
        u = acc[:, pl.ds(pl.multiple_of(U + b * 256, 256), 256)]
        h[:, pl.ds(pl.multiple_of(b * 256, 256), 256)] = (jax.nn.silu(g) * u).astype(BF16)

    @pl.when(d == 1)
    def _():
        h[:, 0:2 * U - FF] = jnp.zeros((2 * ROWS, 2 * U - FF), BF16)

    def swap(n):
        return remote(msend.at[n], mrecv.at[n], out_m, n, mate)

    def cross_y(n):
        return remote(ysend.at[n], yrecv.at[n], out_y, n, ypeer)

    def cross_x(n):
        return remote(xsend.at[n], xrecv.at[n], out_x, n, xpeer)

    def give(n, core):
        cols = pl.ds(pl.multiple_of(n * NC + core * HC, HC), HC)
        return remote(o.at[:, cols], o.at[:, cols], out_o, n, mate)

    @pl.loop(0, NN + LAG_X)
    def _(n):
        @pl.when(n < NN)
        def _():
            s = n % DS
            down(n, 0).wait()
            down(n, 1).wait()
            p = jnp.dot(h[...], dn[s], preferred_element_type=F32)
            mine[n] = p[:, :HC]
            msend[n] = p[:, HC:].astype(BF16)
            swap(n).start()

            @pl.when(n + DS < NN)
            def _():
                down(n + DS, 0).start()
                down(n + DS, 1).start()

        @pl.when(jnp.logical_and(n >= 1, n < NN + 1))
        def _():
            m = n - 1
            swap(m).wait_recv()
            both = mine[m] + mrecv[m].astype(F32)
            ysend[m] = both[ROWS:].astype(BF16)
            mine[m, pl.ds(0, ROWS)] = both[:ROWS]
            cross_y(m).start()

        @pl.when(jnp.logical_and(n >= LAG_Y, n < NN + LAG_Y))
        def _():
            m = n - LAG_Y
            cross_y(m).wait_recv()
            xsend[m] = (mine[m, pl.ds(0, ROWS)] + yrecv[m].astype(F32)).astype(BF16)
            cross_x(m).start()

        @pl.when(n >= LAG_X)
        def _():
            m = n - LAG_X
            cross_x(m).wait_recv()
            cols = pl.ds(pl.multiple_of(m * NC + c * HC, HC), HC)
            o[:, cols] = (xsend[m].astype(F32) + xrecv[m].astype(F32)).astype(BF16)
            give(m, c).start()

    for j in range(5):
        send_y(j).wait_send()
        relay_x(j).wait_send()
        to_mate(j, 0).wait_send()
        to_mate(j, 1).wait_send()

    @pl.loop(0, NN)
    def _(n):
        swap(n).wait_send()
        cross_y(n).wait_send()
        cross_x(n).wait_send()
        give(n, c).wait_send()
        give(n, 1 - c).wait_recv()


def solution(mesh):
    dma = pltpu.SemaphoreType.DMA
    vmem = pltpu.VMEM

    def step(x, w_gate, w_up, w_down):
        return pl.pallas_call(
            kernel,
            out_shape=jax.ShapeDtypeStruct((ROWS, D), BF16),
            in_specs=[pl.BlockSpec(memory_space=pl.ANY)] * 4,
            out_specs=pl.BlockSpec(memory_space=pltpu.VMEM),
            scratch_shapes=[
                vmem((NK, 2 * ROWS, KC), BF16),
                vmem((2 * ROWS, 2 * U), F32),
                vmem((2 * ROWS, U), BF16),
                vmem((GS, 2, KC, U), BF16),
                vmem((DS, U, NC), BF16),
                vmem((NN, 2 * ROWS, HC), F32),
                vmem((NN, 2 * ROWS, HC), BF16),
                vmem((NN, 2 * ROWS, HC), BF16),
                vmem((NN, ROWS, HC), BF16),
                vmem((NN, ROWS, HC), BF16),
                vmem((NN, ROWS, HC), BF16),
                vmem((NN, ROWS, HC), BF16),
                dma((NK,)),
                dma((GS, 2)),
                dma((DS, 2)),
                dma((2, 5)),
                dma((2, 5)),
                dma((2, 10)),
                dma((2, NN)),
                dma((2, NN)),
                dma((2, NN)),
                dma((2, NN)),
            ],
            compiler_params=pltpu.CompilerParams(
                collective_id=0, has_side_effects=True, vmem_limit_bytes=63 * 2**20),
        )(x, w_gate, w_up, w_down)

    return jax.shard_map(
        step,
        mesh=mesh,
        in_specs=(P("dp", None), P(None, "tp"), P(None, "tp"), P("tp", None)),
        out_specs=P("dp", None),
        check_vma=False,
    )
```

```python
import jax
import jax.numpy as jnp
from jax import lax
from jax.experimental import pallas as pl
from jax.experimental.pallas import tpu as pltpu
from jax.sharding import PartitionSpec as P

MESH = pl.DeviceIdType.MESH
ROWS, D, FF = 128, 5120, 4480
U = 2304
SKIP = FF - U
KC = 512
NK = D // KC
NC = 512
NN = D // NC
HC = NC // 2
GS = 6
DS = 4
LAG_Y, LAG_X = 5, 7
F32, BF16 = jnp.float32, jnp.bfloat16


def kernel(x, wg, wu, wd, o, X, acc, h, gu, dn, mine, msend, mrecv, ysend, yrecv, xsend, xrecv,
           fin, xsem, ksem, gsem, dsem, in_y, in_x, in_m, out_m, out_y, out_x, out_o):
    d, t = lax.axis_index("dp"), lax.axis_index("tp")
    xi, c = t // 2, t % 2
    mate, ypeer, xpeer = (d, t + 1 - 2 * c), (1 - d, t), (d, (t + 2) % 4)
    unit0 = pl.multiple_of(d * SKIP, 128)

    def remote(src, dst, sems, i, peer):
        return pltpu.make_async_remote_copy(
            src_ref=src, dst_ref=dst, send_sem=sems.at[0, i], recv_sem=sems.at[1, i], device_id=peer, device_id_type=MESH)

    def chunk(i):
        pair = (i - 2) // 2
        j = jnp.where(i < 2, i, jnp.where(i < 8, jnp.where(i % 2 == 0, pair + 2, pair), i - 5))
        relayed = jnp.where(i < 8, jnp.where(i < 2, 0, i % 2), 1)
        return 2 * j + jnp.where(relayed == 1, 1 - xi, xi)

    def x_own(k):
        return pltpu.make_async_copy(x.at[:, pl.ds(k * KC, KC)], X.at[k, pl.ds(0, ROWS)], xsem.at[k])

    def slab(i, which):
        w = (wg, wu)[which]
        rows = pl.ds(pl.multiple_of(chunk(i) * KC, KC), KC)
        s = i % GS
        return pltpu.make_async_copy(w.at[rows, pl.ds(unit0, U)], gu.at[s, which], gsem.at[s, which])

    def down(n, half):
        s = n % DS
        cols = pl.ds(pl.multiple_of(n * NC + jnp.where(half == 0, c, 1 - c) * HC, HC), HC)
        return pltpu.make_async_copy(
            wd.at[pl.ds(unit0, U), cols], dn.at[s, :, pl.ds(half * HC, HC)], dsem.at[s, half])

    def other(k, core):
        return X.at[k, pl.ds(ROWS, ROWS), pl.ds(pl.multiple_of(core * (KC // 2), KC // 2), KC // 2)]

    def mine_x(k):
        return X.at[k, pl.ds(0, ROWS), pl.ds(pl.multiple_of(c * (KC // 2), KC // 2), KC // 2)]

    def send_y(j):
        return remote(mine_x(2 * j + xi), other(2 * j + xi, c), in_y, j, ypeer)

    def relay_x(j):
        return remote(other(2 * j + xi, c), other(2 * j + xi, c), in_x, j, xpeer)

    def got_x(j):
        return remote(other(2 * j + 1 - xi, c), other(2 * j + 1 - xi, c), in_x, j, xpeer)

    def to_mate(j, relayed):
        k = 2 * j + (1 - xi if relayed else xi)
        return remote(other(k, c), other(k, c), in_m, j + 5 * relayed, mate)

    def from_mate(j, relayed):
        k = 2 * j + (1 - xi if relayed else xi)
        return remote(other(k, 1 - c), other(k, 1 - c), in_m, j + 5 * relayed, mate)

    for k in range(NK):
        x_own(k).start()
    for i in range(GS):
        slab(i, 0).start(priority=1)
        slab(i, 1).start(priority=1)
    barrier = pltpu.get_barrier_semaphore()
    for peer in (mate, ypeer, xpeer):
        pl.semaphore_signal(barrier, inc=1, device_id=peer, device_id_type=MESH)
    acc[...] = jnp.zeros_like(acc)
    with jax.named_scope("bar"):
        pl.semaphore_wait(barrier, 3)
    with jax.named_scope("wxown"):
        for k in range(NK):
            x_own(k).wait()
    for j in range(5):
        send_y(j).start()
    for n in range(DS):
        down(n, 0).start(priority=1)
        down(n, 1).start(priority=1)

    def direct(j):
        with jax.named_scope("wdirect"):
            send_y(j).wait_recv()
        relay_x(j).start()
        to_mate(j, 0).start()

    def relayed(j):
        with jax.named_scope("wrelay"):
            got_x(j).wait_recv()
        to_mate(j, 1).start()

    def whole(j, was_relayed):
        with jax.named_scope("wmate"):
            from_mate(j, was_relayed).wait_recv()

    def arrived(i):
        with jax.named_scope("wslab"):
            slab(i, 0).wait()
            slab(i, 1).wait()

    def free(i):
        @pl.when(i + GS < NK)
        def _():
            slab(i + GS, 0).start(priority=1)
            slab(i + GS, 1).start(priority=1)

    def multiply(i, rows):
        xk = X[chunk(i), rows]
        with jax.named_scope("dot1"):
            for which in range(2):
                acc[rows, which * U:(which + 1) * U] += jnp.dot(xk, gu[i % GS, which], preferred_element_type=F32)

    own, others, both = slice(0, ROWS), slice(ROWS, 2 * ROWS), slice(0, 2 * ROWS)

    @pl.loop(0, 3)
    def _(i):
        arrived(i)
        multiply(i, own)

        @pl.when(i == 1)
        def _():
            direct(0)

    @pl.loop(0, 3)
    def _(i):
        @pl.when(i < 2)
        def _():
            direct(i + 1)

        @pl.when(i == 2)
        def _():
            relayed(0)

        whole(i, 0)
        multiply(i, others)
        free(i)

    @pl.loop(3, NK)
    def _(i):
        @pl.when(i < 5)
        def _():
            direct(i)
            relayed(i - 2)

        @pl.when(jnp.logical_and(i >= 5, i < 7))
        def _():
            relayed(i - 2)

        @pl.when(i % 2 == 1)
        def _():
            @pl.when(i < 9)
            def _():
                whole((i - 3) // 2, 1)

            @pl.when(i == 9)
            def _():
                whole(4, 1)

        @pl.when(i % 2 == 0)
        def _():
            @pl.when(i < 8)
            def _():
                whole(i // 2 + 1, 0)

            @pl.when(i == 8)
            def _():
                whole(3, 1)

        arrived(i)
        multiply(i, both)
        free(i)

    @pl.loop(0, U // 256)
    def _(b):
        g = acc[:, pl.ds(pl.multiple_of(b * 256, 256), 256)]
        u = acc[:, pl.ds(pl.multiple_of(U + b * 256, 256), 256)]
        h[:, pl.ds(pl.multiple_of(b * 256, 256), 256)] = (jax.nn.silu(g) * u).astype(BF16)

    @pl.when(d == 1)
    def _():
        h[:, 0:2 * U - FF] = jnp.zeros((2 * ROWS, 2 * U - FF), BF16)

    def swap(n):
        return remote(msend.at[n], mrecv.at[n], out_m, n, mate)

    def cross_y(n):
        return remote(ysend.at[n], yrecv.at[n], out_y, n, ypeer)

    def cross_x(n):
        return remote(xsend.at[n], xrecv.at[n], out_x, n, xpeer)

    def give(n, core):
        cols = pl.ds(pl.multiple_of(n * NC + core * HC, HC), HC)
        return remote(fin.at[n], o.at[:, cols], out_o, n, mate)

    def keep(n):
        return pltpu.make_async_copy(fin.at[n], o.at[:, pl.ds(pl.multiple_of(n * NC + c * HC, HC), HC)], ksem.at[n])

    @pl.loop(0, NN + LAG_X)
    def _(n):
        @pl.when(n < NN)
        def _():
            s = n % DS
            with jax.named_scope('wdown'):
                down(n, 0).wait()
                down(n, 1).wait()
            with jax.named_scope('dot2'):
                p = jnp.dot(h[...], dn[s], preferred_element_type=F32)
            mine[n] = p[:, :HC]
            msend[n] = p[:, HC:].astype(BF16)
            swap(n).start()

            @pl.when(n + DS < NN)
            def _():
                down(n + DS, 0).start(priority=1)
                down(n + DS, 1).start(priority=1)

        @pl.when(jnp.logical_and(n >= 1, n < NN + 1))
        def _():
            m = n - 1
            with jax.named_scope('wswap'):
                swap(m).wait_recv()
            both = mine[m] + mrecv[m].astype(F32)
            ysend[m] = both[ROWS:].astype(BF16)
            mine[m, pl.ds(0, ROWS)] = both[:ROWS]
            cross_y(m).start()

        @pl.when(jnp.logical_and(n >= LAG_Y, n < NN + LAG_Y))
        def _():
            m = n - LAG_Y
            with jax.named_scope('wy'):
                cross_y(m).wait_recv()
            xsend[m] = (mine[m, pl.ds(0, ROWS)] + yrecv[m].astype(F32)).astype(BF16)
            cross_x(m).start()

        @pl.when(n >= LAG_X)
        def _():
            m = n - LAG_X
            with jax.named_scope('wx'):
                cross_x(m).wait_recv()
            fin[m] = (xsend[m].astype(F32) + xrecv[m].astype(F32)).astype(BF16)
            give(m, c).start()
            keep(m).start()

    for j in range(5):
        send_y(j).wait_send()
        relay_x(j).wait_send()
        to_mate(j, 0).wait_send()
        to_mate(j, 1).wait_send()

    @pl.loop(0, NN)
    def _(n):
        swap(n).wait_send()
        cross_y(n).wait_send()
        cross_x(n).wait_send()
        keep(n).wait()
        give(n, c).wait_send()
        give(n, 1 - c).wait_recv()


def solution(mesh):
    dma = pltpu.SemaphoreType.DMA
    vmem = pltpu.VMEM

    def step(x, w_gate, w_up, w_down):
        return pl.pallas_call(
            kernel,
            out_shape=jax.ShapeDtypeStruct((ROWS, D), BF16),
            in_specs=[pl.BlockSpec(memory_space=pl.ANY)] * 4,
            out_specs=pl.BlockSpec(memory_space=pl.ANY),
            scratch_shapes=[
                vmem((NK, 2 * ROWS, KC), BF16),
                vmem((2 * ROWS, 2 * U), F32),
                vmem((2 * ROWS, U), BF16),
                vmem((GS, 2, KC, U), BF16),
                vmem((DS, U, NC), BF16),
                vmem((NN, 2 * ROWS, HC), F32),
                vmem((NN, 2 * ROWS, HC), BF16),
                vmem((NN, 2 * ROWS, HC), BF16),
                vmem((NN, ROWS, HC), BF16),
                vmem((NN, ROWS, HC), BF16),
                vmem((NN, ROWS, HC), BF16),
                vmem((NN, ROWS, HC), BF16),
                vmem((NN, ROWS, HC), BF16),
                dma((NK,)),
                dma((NN,)),
                dma((GS, 2)),
                dma((DS, 2)),
                dma((2, 5)),
                dma((2, 5)),
                dma((2, 10)),
                dma((2, NN)),
                dma((2, NN)),
                dma((2, NN)),
                dma((2, NN)),
            ],
            compiler_params=pltpu.CompilerParams(
                collective_id=0, has_side_effects=True, vmem_limit_bytes=63 * 2**20),
        )(x, w_gate, w_up, w_down)

    return jax.shard_map(
        step,
        mesh=mesh,
        in_specs=(P("dp", None), P(None, "tp"), P(None, "tp"), P("tp", None)),
        out_specs=P("dp", None),
        check_vma=False,
    )
```

```python
import jax
import jax.numpy as jnp
from jax import lax
from jax.experimental import pallas as pl
from jax.experimental.pallas import tpu as pltpu
from jax.sharding import PartitionSpec as P

MESH = pl.DeviceIdType.MESH
ROWS, D, FF = 128, 5120, 4480
U = 2304
SKIP = FF - U
KC = 512
NK = D // KC
NC = 512
NN = D // NC
HC = NC // 2
GS = 6
DS = 5
LAG_O, LAG_Y, LAG_X = 2, 3, 6
F32, BF16 = jnp.float32, jnp.bfloat16


def kernel(x, wg, wu, wd, o, xs, acc, h, gu, dn, xkeep, okeep, xpart, xgot, opart, ogot, ysend, yrecv, xsend, xrecv,
           xsem, gsem, dsem, in_y, in_x, in_m, sx, so, out_y, out_x, out_o):
    d, t = lax.axis_index("dp"), lax.axis_index("tp")
    xi, c = t // 2, t % 2
    mate, ypeer, xpeer = (d, t + 1 - 2 * c), (1 - d, t), (d, (t + 2) % 4)
    unit0 = pl.multiple_of(d * SKIP, 128)

    def remote(src, dst, sems, i, peer):
        return pltpu.make_async_remote_copy(
            src_ref=src, dst_ref=dst, send_sem=sems.at[sems.shape[0] - 1], recv_sem=sems.at[i],
            device_id=peer, device_id_type=MESH)

    def all_sent(sems):
        n = sems.shape[0] - 1
        pltpu.make_async_copy(xpart.at[pl.ds(0, n)], xpart.at[pl.ds(0, n)], sems.at[n]).wait()

    def chunk(i):
        pair = (i - 2) // 2
        j = jnp.where(i < 2, i, jnp.where(i < 8, jnp.where(i % 2 == 0, pair + 2, pair), i - 5))
        relayed = jnp.where(i < 8, jnp.where(i < 2, 0, i % 2), 1)
        return 2 * j + jnp.where(relayed == 1, 1 - xi, xi)

    def x_own(k):
        return pltpu.make_async_copy(x.at[:, pl.ds(k * KC, KC)], xs.at[k, pl.ds(0, ROWS)], xsem.at[0])

    def slab(i, which):
        w = (wg, wu)[which]
        rows = pl.ds(pl.multiple_of(chunk(i) * KC, KC), KC)
        s = i % GS
        return pltpu.make_async_copy(w.at[rows, pl.ds(unit0, U)], gu.at[s, which], gsem.at[s])

    def down(n, half):
        s = n % DS
        cols = pl.ds(pl.multiple_of(n * NC + jnp.where(half == 0, c, 1 - c) * HC, HC), HC)
        return pltpu.make_async_copy(
            wd.at[pl.ds(unit0, U), cols], dn.at[s, :, pl.ds(half * HC, HC)], dsem.at[s])

    def load(n):
        down(n, 0).start(priority=1)
        down(n, 1).start(priority=1)

    def other(k, core):
        return xs.at[k, pl.ds(ROWS, ROWS), pl.ds(pl.multiple_of(core * (KC // 2), KC // 2), KC // 2)]

    def mine_x(k):
        return xs.at[k, pl.ds(0, ROWS), pl.ds(pl.multiple_of(c * (KC // 2), KC // 2), KC // 2)]

    def send_y(j):
        return remote(mine_x(2 * j + xi), other(2 * j + xi, c), in_y, j, ypeer)

    def relay_x(j):
        return remote(other(2 * j + xi, c), other(2 * j + xi, c), in_x, j, xpeer)

    def got_x(j):
        return remote(other(2 * j + 1 - xi, c), other(2 * j + 1 - xi, c), in_x, j, xpeer)

    def to_mate(j, relayed):
        k = 2 * j + (1 - xi if relayed else xi)
        return remote(other(k, c), other(k, c), in_m, j + 5 * relayed, mate)

    def from_mate(j, relayed):
        k = 2 * j + (1 - xi if relayed else xi)
        return remote(other(k, 1 - c), other(k, 1 - c), in_m, j + 5 * relayed, mate)

    for k in range(NK):
        x_own(k).start()
    for i in range(GS):
        slab(i, 0).start(priority=1)
        slab(i, 1).start(priority=1)
    barrier = pltpu.get_barrier_semaphore()
    for peer in (mate, ypeer, xpeer):
        pl.semaphore_signal(barrier, inc=1, device_id=peer, device_id_type=MESH)
    acc[...] = jnp.zeros_like(acc)
    with jax.named_scope("bar"):
        pl.semaphore_wait(barrier, 3)
    with jax.named_scope("wxown"):
        pltpu.make_async_copy(x, o, xsem.at[0]).wait()
    for j in range(5):
        send_y(j).start()
    def direct(j):
        with jax.named_scope("wdirect"):
            send_y(j).wait_recv()
        relay_x(j).start()
        to_mate(j, 0).start()

    def relayed(j):
        with jax.named_scope("wrelay"):
            got_x(j).wait_recv()
        to_mate(j, 1).start()

    def whole(j, was_relayed):
        with jax.named_scope("wmate"):
            from_mate(j, was_relayed).wait_recv()

    here = set()

    def arrived(i):
        if i in here:
            return
        here.add(i)
        with jax.named_scope("wslab"):
            pltpu.make_async_copy(gu.at[i % GS], gu.at[i % GS], gsem.at[i % GS]).wait()

    def free(i):
        if i + GS < NK:
            slab(i + GS, 0).start(priority=1)
            slab(i + GS, 1).start(priority=1)

    def multiply(i, rows):
        xk = xs[chunk(i), rows]
        with jax.named_scope("dot1"):
            for which in range(2):
                acc[rows, which * U:(which + 1) * U] += jnp.dot(xk, gu[i % GS, which], preferred_element_type=F32)

    own, others, both = slice(0, ROWS), slice(ROWS, 2 * ROWS), slice(0, 2 * ROWS)
    relayed_ones = {3: 0, 5: 1, 7: 2, 8: 3, 9: 4}
    direct_ones = {0: 0, 1: 1, 2: 2, 4: 3, 6: 4}

    def complete(i):
        if i in relayed_ones:
            whole(relayed_ones[i], 1)
        else:
            whole(direct_ones[i], 0)

    def gate(rows):
        with jax.named_scope("silu"):
            @pl.loop(0, U // 256)
            def _(b):
                g = acc[rows, pl.ds(pl.multiple_of(b * 256, 256), 256)]
                u = acc[rows, pl.ds(pl.multiple_of(U + b * 256, 256), 256)]
                h[rows, pl.ds(pl.multiple_of(b * 256, 256), 256)] = (jax.nn.silu(g) * u).astype(BF16)

        @pl.when(d == 1)
        def _():
            h[rows, 0:2 * U - FF] = jnp.zeros((ROWS, 2 * U - FF), BF16)

    def O(*steps):
        for i in steps:
            arrived(i)
        for i in steps:
            multiply(i, own)

    def X(*steps):
        for i in steps:
            complete(i)
        for i in steps:
            arrived(i)
        for i in steps:
            multiply(i, others)

    def F(*steps):
        for i in steps:
            complete(i)
        for i in steps:
            arrived(i)
        for i in steps:
            multiply(i, both)

    def swap_x(n):
        return remote(xpart.at[n], xgot.at[n], sx, n, mate)

    def swap_o(n):
        return remote(opart.at[n], ogot.at[n], so, n, mate)

    def cross_y(n):
        return remote(ysend.at[n], yrecv.at[n], out_y, n, ypeer)

    def cross_x(n):
        return remote(xsend.at[n], xrecv.at[n], out_x, n, xpeer)

    def give(n, core):
        cols = pl.ds(pl.multiple_of(n * NC + core * HC, HC), HC)
        return remote(o.at[:, cols], o.at[:, cols], out_o, n, mate)

    def product(n, rows, keep, part, swap):
        with jax.named_scope("dot2"):
            p = jnp.dot(h[rows], dn[n % DS], preferred_element_type=F32)
            keep[n] = p[:, :HC]
            part[n] = p[:, HC:].astype(BF16)
        swap(n).start()

    def product_x(n):
        with jax.named_scope("wdown"):
            pltpu.make_async_copy(dn.at[n % DS], dn.at[n % DS], dsem.at[n % DS]).wait()
        product(n, others, xkeep, xpart, swap_x)

    def product_o(n):
        product(n, own, okeep, opart, swap_o)

        @pl.when(n + DS < NN)
        def _():
            load(n + DS)

    def pass_y(n):
        with jax.named_scope("wswap"):
            swap_x(n).wait_recv()
        ysend[n] = (xkeep[n] + xgot[n].astype(F32)).astype(BF16)
        cross_y(n).start()

    def pass_x(n):
        swap_o(n).wait_recv()
        with jax.named_scope("wy"):
            cross_y(n).wait_recv()
        xsend[n] = (okeep[n] + ogot[n].astype(F32) + yrecv[n].astype(F32)).astype(BF16)
        cross_x(n).start()

    def finish(n):
        with jax.named_scope("wx"):
            cross_x(n).wait_recv()
        cols = pl.ds(pl.multiple_of(n * NC + c * HC, HC), HC)
        o[:, cols] = (xsend[n].astype(F32) + xrecv[n].astype(F32)).astype(BF16)
        give(n, c).start()

    O(0)
    O(1)
    direct(0)
    O(2)
    direct(1)
    X(0)
    free(0)
    O(3)
    direct(2)
    X(1)
    free(1)
    relayed(0)
    X(2)
    free(2)
    direct(3)
    relayed(1)
    X(3)
    free(3)
    direct(4)
    F(4)
    relayed(2)
    F(5)
    relayed(3)
    F(6)
    load(0)
    relayed(4)
    X(7)
    load(1)
    X(8)
    load(2)
    X(9)
    load(3)
    load(4)
    gate(others)
    product_x(0)
    product_x(1)
    O(7)
    pass_y(0)
    pass_y(1)
    product_x(2)
    O(8)
    pass_y(2)
    O(9)
    gate(own)
    product_o(0)
    product_x(3)
    product_o(1)
    pass_x(0)

    @pl.loop(4, NN + LAG_X)
    def _(n):
        @pl.when(n < NN)
        def _():
            product_x(n)

        @pl.when(n < NN + 1)
        def _():
            pass_y(n - 1)

        @pl.when(n < NN + LAG_O)
        def _():
            product_o(n - LAG_O)

        @pl.when(n < NN + LAG_Y)
        def _():
            pass_x(n - LAG_Y)

        @pl.when(n >= LAG_X)
        def _():
            finish(n - LAG_X)

    with jax.named_scope("wgive"):
        @pl.loop(0, NN)
        def _(n):
            give(n, 1 - c).wait_recv()

    with jax.named_scope("wend"):
        for sems in (in_y, in_x, in_m, sx, so, out_y, out_x, out_o):
            all_sent(sems)


def solution(mesh):
    dma = pltpu.SemaphoreType.DMA
    vmem = pltpu.VMEM

    def step(x, w_gate, w_up, w_down):
        return pl.pallas_call(
            kernel,
            out_shape=pltpu.VMEM((ROWS, D), BF16),
            in_specs=[pl.BlockSpec(memory_space=pl.ANY)] * 4,
            out_specs=pl.BlockSpec(memory_space=pltpu.VMEM),
            scratch_shapes=[
                vmem((NK, 2 * ROWS, KC), BF16),
                vmem((2 * ROWS, 2 * U), F32),
                vmem((2 * ROWS, U), BF16),
                vmem((GS, 2, KC, U), BF16),
                vmem((DS, U, NC), BF16),
                vmem((NN, ROWS, HC), F32),
                vmem((NN, ROWS, HC), F32),
                *[vmem((NN, ROWS, HC), BF16)] * 8,
                dma((1,)),
                dma((GS,)),
                dma((DS,)),
                dma((6,)),
                dma((6,)),
                dma((11,)),
                *[dma((NN + 1,))] * 5,
            ],
            compiler_params=pltpu.CompilerParams(
                collective_id=0, has_side_effects=True, vmem_limit_bytes=60 * 2**20),
        )(x, w_gate, w_up, w_down)

    return jax.shard_map(
        step,
        mesh=mesh,
        in_specs=(P("dp", None), P(None, "tp"), P(None, "tp"), P("tp", None)),
        out_specs=P("dp", None),
        check_vma=False,
    )
```

```python
import jax
import jax.numpy as jnp
from jax import lax
from jax.experimental import pallas as pl
from jax.experimental.pallas import tpu as pltpu
from jax.sharding import PartitionSpec as P

MESH = pl.DeviceIdType.MESH
ROWS, D, FF = 128, 5120, 4480
U = 2304
SKIP = FF - U
KC = 512
NK = D // KC
NC = 512
NN = D // NC
HC = NC // 2
GS = 6
DS = 6
LAG_Y, LAG_X = 3, 6
F32, BF16 = jnp.float32, jnp.bfloat16


def kernel(x, wg, wu, wd, o, xs, acc, h, gu, dn, xkeep, okeep, xpart, xgot, opart, ogot, ysend, yrecv, xsend, xrecv,
           xsem, gsem, dsem, in_y, in_x, in_m, sx, so, out_y, out_x, out_o):
    d, t = lax.axis_index("dp"), lax.axis_index("tp")
    xi, c = t // 2, t % 2
    mate, ypeer, xpeer = (d, t + 1 - 2 * c), (1 - d, t), (d, (t + 2) % 4)
    unit0 = pl.multiple_of(d * SKIP, 128)

    def remote(src, dst, sems, i, peer):
        return pltpu.make_async_remote_copy(
            src_ref=src, dst_ref=dst, send_sem=sems.at[sems.shape[0] - 1], recv_sem=sems.at[i],
            device_id=peer, device_id_type=MESH)

    def all_sent(sems, blocks):
        some = xpart.at[pl.ds(0, blocks)]
        pltpu.make_async_copy(some, some, sems.at[sems.shape[0] - 1]).wait()

    def chunk(i):
        pair = (i - 2) // 2
        j = jnp.where(i < 2, i, jnp.where(i < 8, jnp.where(i % 2 == 0, pair + 2, pair), i - 5))
        relayed = jnp.where(i < 8, jnp.where(i < 2, 0, i % 2), 1)
        return 2 * j + jnp.where(relayed == 1, 1 - xi, xi)

    def x_own(k):
        return pltpu.make_async_copy(x.at[:, pl.ds(k * KC, KC)], xs.at[k, pl.ds(0, ROWS)], xsem.at[0])

    def slab(i, which):
        w = (wg, wu)[which]
        rows = pl.ds(pl.multiple_of(chunk(i) * KC, KC), KC)
        s = i % GS
        return pltpu.make_async_copy(w.at[rows, pl.ds(unit0, U)], gu.at[s, which], gsem.at[s, which])

    def down(n, half):
        s = n % DS
        cols = pl.ds(pl.multiple_of(n * NC + jnp.where(half == 0, c, 1 - c) * HC, HC), HC)
        return pltpu.make_async_copy(
            wd.at[pl.ds(unit0, U), cols], dn.at[s, :, pl.ds(half * HC, HC)], dsem.at[s])

    def load(n):
        down(n, 0).start(priority=1)
        down(n, 1).start(priority=1)

    def other(k, core):
        return xs.at[k, pl.ds(ROWS, ROWS), pl.ds(pl.multiple_of(core * (KC // 2), KC // 2), KC // 2)]

    def mine_x(k):
        return xs.at[k, pl.ds(0, ROWS), pl.ds(pl.multiple_of(c * (KC // 2), KC // 2), KC // 2)]

    def send_y(j):
        return remote(mine_x(2 * j + xi), other(2 * j + xi, c), in_y, j, ypeer)

    def relay_x(j):
        return remote(other(2 * j + xi, c), other(2 * j + xi, c), in_x, j, xpeer)

    def got_x(j):
        return remote(other(2 * j + 1 - xi, c), other(2 * j + 1 - xi, c), in_x, j, xpeer)

    def to_mate(j, relayed):
        k = 2 * j + (1 - xi if relayed else xi)
        return remote(other(k, c), other(k, c), in_m, j + 5 * relayed, mate)

    def from_mate(j, relayed):
        k = 2 * j + (1 - xi if relayed else xi)
        return remote(other(k, 1 - c), other(k, 1 - c), in_m, j + 5 * relayed, mate)

    for k in range(NK):
        x_own(k).start()
    for i in range(GS):
        slab(i, 0).start(priority=1)
        slab(i, 1).start(priority=1)
    barrier = pltpu.get_barrier_semaphore()
    for peer in (mate, ypeer, xpeer):
        pl.semaphore_signal(barrier, inc=1, device_id=peer, device_id_type=MESH)
    acc[...] = jnp.zeros_like(acc)
    with jax.named_scope("bar"):
        pl.semaphore_wait(barrier, 3)
    with jax.named_scope("wxown"):
        pltpu.make_async_copy(x, o, xsem.at[0]).wait()
    for j in range(5):
        send_y(j).start()
    def direct(j):
        with jax.named_scope("wdirect"):
            send_y(j).wait_recv()
        relay_x(j).start()
        to_mate(j, 0).start()

    def relayed(j):
        with jax.named_scope("wrelay"):
            got_x(j).wait_recv()
        to_mate(j, 1).start()

    def whole(j, was_relayed):
        with jax.named_scope("wmate"):
            from_mate(j, was_relayed).wait_recv()

    here = set()

    def arrived(i):
        if i in here:
            return
        here.add(i)
        with jax.named_scope("wslab"):
            slab(i, 0).wait()
            slab(i, 1).wait()

    def free(i):
        if i + GS < NK:
            slab(i + GS, 0).start(priority=1)
            slab(i + GS, 1).start(priority=1)

    def multiply(i, rows):
        xk = xs[chunk(i), rows]
        with jax.named_scope("dot1"):
            for which in range(2):
                acc[rows, which * U:(which + 1) * U] += jnp.dot(xk, gu[i % GS, which], preferred_element_type=F32)

    own, others, both = slice(0, ROWS), slice(ROWS, 2 * ROWS), slice(0, 2 * ROWS)
    relayed_ones = {3: 0, 5: 1, 7: 2, 8: 3, 9: 4}
    direct_ones = {0: 0, 1: 1, 2: 2, 4: 3, 6: 4}

    def complete(i):
        if i in relayed_ones:
            whole(relayed_ones[i], 1)
        else:
            whole(direct_ones[i], 0)

    def last(i, rows):
        xk = xs[chunk(i), rows]
        with jax.named_scope("dot1last"):
            for b in range(U // 256):
                gate, up = (
                    acc[rows, w * U + b * 256:w * U + (b + 1) * 256]
                    + jnp.dot(xk, gu[i % GS, w, :, b * 256:(b + 1) * 256], preferred_element_type=F32)
                    for w in range(2))
                h[rows, b * 256:(b + 1) * 256] = (jax.nn.silu(gate) * up).astype(BF16)

        @pl.when(d == 1)
        def _():
            h[rows, 0:2 * U - FF] = jnp.zeros((ROWS, 2 * U - FF), BF16)

    def O(*steps):
        for i in steps:
            arrived(i)
        for i in steps:
            multiply(i, own)

    def O_in_parts(i):
        here.add(i)
        xk = xs[chunk(i), own]
        for which in range(2):
            slab(i, which).wait()
            with jax.named_scope("dot1h"):
                acc[own, which * U:(which + 1) * U] += jnp.dot(xk, gu[i % GS, which], preferred_element_type=F32)

    def X(*steps):
        for i in steps:
            complete(i)
        for i in steps:
            arrived(i)
        for i in steps:
            multiply(i, others)

    def F(*steps):
        for i in steps:
            complete(i)
        for i in steps:
            arrived(i)
        for i in steps:
            multiply(i, both)

    def swap_x(n):
        return remote(xpart.at[n], xgot.at[n], sx, n, mate)

    def swap_o(n):
        return remote(opart.at[n], ogot.at[n], so, n, mate)

    def part(q):
        return pl.ds(q * (ROWS // 2), ROWS // 2)

    def cross_y(n, q):
        return remote(ysend.at[n, part(q)], yrecv.at[n, part(q)], out_y, 2 * n + q, ypeer)

    def cross_x(n, q):
        return remote(xsend.at[n, part(q)], xrecv.at[n, part(q)], out_x, 2 * n + q, xpeer)

    def give(n, core):
        cols = pl.ds(pl.multiple_of(n * NC + core * HC, HC), HC)
        return remote(o.at[:, cols], o.at[:, cols], out_o, n, mate)

    def loaded(n):
        with jax.named_scope("wdown"):
            pltpu.make_async_copy(dn.at[n % DS], dn.at[n % DS], dsem.at[n % DS]).wait()

    def more(n):
        @pl.when(n + DS < NN)
        def _():
            load(n + DS)

    def product_x(n):
        loaded(n)
        with jax.named_scope("dot2"):
            p = jnp.dot(h[others], dn[n % DS], preferred_element_type=F32)
            xkeep[n] = p[:, :HC]
            xpart[n] = p[:, HC:].astype(BF16)
        swap_x(n).start()

    def product_o(n):
        with jax.named_scope("dot2"):
            p = jnp.dot(h[own], dn[n % DS], preferred_element_type=F32)
            okeep[n] = p[:, :HC]
            opart[n] = p[:, HC:].astype(BF16)
        swap_o(n).start()
        more(n)

    def products(n, m):
        loaded(n)
        with jax.named_scope("dot2b"):
            p = jnp.dot(h[others], dn[n % DS], preferred_element_type=F32)
            r = jnp.dot(h[own], dn[m % DS], preferred_element_type=F32)
            xkeep[n] = p[:, :HC]
            xpart[n] = p[:, HC:].astype(BF16)
            okeep[m] = r[:, :HC]
            opart[m] = r[:, HC:].astype(BF16)
        swap_x(n).start()
        swap_o(m).start()
        more(m)

    def pass_y(n):
        with jax.named_scope("wswap"):
            swap_x(n).wait_recv()
        ysend[n] = (xkeep[n] + xgot[n].astype(F32)).astype(BF16)
        cross_y(n, 0).start()
        cross_y(n, 1).start()

    def pass_x(n, q):
        if q == 0:
            with jax.named_scope("wswapo"):
                swap_o(n).wait_recv()
        with jax.named_scope("wy"):
            cross_y(n, q).wait_recv()
        r = part(q)
        xsend[n, r] = (okeep[n, r] + ogot[n, r].astype(F32) + yrecv[n, r].astype(F32)).astype(BF16)
        cross_x(n, q).start()

    def finish(n):
        with jax.named_scope("wx"):
            cross_x(n, 0).wait_recv()
            cross_x(n, 1).wait_recv()
        cols = pl.ds(pl.multiple_of(n * NC + c * HC, HC), HC)
        o[:, cols] = (xsend[n].astype(F32) + xrecv[n].astype(F32)).astype(BF16)
        give(n, c).start()

    O(0)
    O(1)
    direct(0)
    O_in_parts(2)
    direct(1)
    X(0)
    free(0)
    O(3)
    direct(2)
    X(1)
    free(1)
    relayed(0)
    X(2)
    free(2)
    direct(3)
    X(3)
    free(3)
    relayed(1)
    direct(4)
    O(4)
    X(4)
    relayed(2)
    F(5)
    relayed(3)
    F(6)
    load(0)
    relayed(4)
    X(7)
    load(1)
    X(8)
    load(2)
    complete(9)
    arrived(9)
    last(9, others)
    for n in range(3, DS):
        load(n)
    product_x(0)
    O(7)
    product_x(1)
    pass_y(0)
    O(8)
    product_x(2)
    pass_y(1)
    last(9, own)
    pass_y(2)
    product_o(0)
    products(3, 1)

    @pl.loop(LAG_Y, NN + LAG_X)
    def _(n):
        @pl.when(n < NN + LAG_Y)
        def _():
            pass_x(n - LAG_Y, 0)

        @pl.when(n < NN - 1)
        def _():
            products(n + 1, n - 1)

        @pl.when(jnp.logical_and(n >= NN - 1, n < NN + 1))
        def _():
            product_o(n - 1)

        @pl.when(n < NN)
        def _():
            pass_y(n)

        @pl.when(n < NN + LAG_Y)
        def _():
            pass_x(n - LAG_Y, 1)

        @pl.when(n >= LAG_X)
        def _():
            finish(n - LAG_X)

    with jax.named_scope("wgive"):
        @pl.loop(0, NN)
        def _(n):
            give(n, 1 - c).wait_recv()

    with jax.named_scope("wend"):
        for sems in (in_y, in_x):
            all_sent(sems, 5)
        for sems in (in_m, sx, so, out_y, out_x, out_o):
            all_sent(sems, NN)


def solution(mesh):
    dma = pltpu.SemaphoreType.DMA
    vmem = pltpu.VMEM

    def step(x, w_gate, w_up, w_down):
        return pl.pallas_call(
            kernel,
            out_shape=pltpu.VMEM((ROWS, D), BF16),
            in_specs=[pl.BlockSpec(memory_space=pl.ANY)] * 4,
            out_specs=pl.BlockSpec(memory_space=pltpu.VMEM),
            scratch_shapes=[
                vmem((NK, 2 * ROWS, KC), BF16),
                vmem((2 * ROWS, 2 * U), F32),
                vmem((2 * ROWS, U), BF16),
                vmem((GS, 2, KC, U), BF16),
                vmem((DS, U, NC), BF16),
                vmem((NN, ROWS, HC), F32),
                vmem((NN, ROWS, HC), F32),
                *[vmem((NN, ROWS, HC), BF16)] * 8,
                dma((1,)),
                dma((GS, 2)),
                dma((DS,)),
                dma((6,)),
                dma((6,)),
                dma((11,)),
                *[dma((NN + 1,))] * 2,
                *[dma((2 * NN + 1,))] * 2,
                dma((NN + 1,)),
            ],
            compiler_params=pltpu.CompilerParams(
                collective_id=0, has_side_effects=True, vmem_limit_bytes=61 * 2**20),
        )(x, w_gate, w_up, w_down)

    return jax.shard_map(
        step,
        mesh=mesh,
        in_specs=(P("dp", None), P(None, "tp"), P(None, "tp"), P("tp", None)),
        out_specs=P("dp", None),
        check_vma=False,
    )
```

```python
import jax
import jax.numpy as jnp
from jax import lax
from jax.experimental import pallas as pl
from jax.experimental.pallas import tpu as pltpu
from jax.sharding import PartitionSpec as P

MESH = pl.DeviceIdType.MESH
ROWS, D, FF = 128, 5120, 4480
U = 2304
SKIP = FF - U
KC = 512
NK = D // KC
NC = 512
NN = D // NC
HC = NC // 2
GS = 6
DS = 6
LAG_Y, LAG_X = 3, 6
RING, RING_Y = 4, 7
F32, BF16 = jnp.float32, jnp.bfloat16


def kernel(x, wg, wu, wd, o, xs, acc, h, gu, dn, xkeep, okeep, xpart, xgot, opart, ogot, ysend, yrecv, xsend, xrecv,
           xsem, gsem, dsem, in_y, in_x, in_m, sx, so, out_y, out_x, out_o):
    d, t = lax.axis_index("dp"), lax.axis_index("tp")
    xi, c = t // 2, t % 2
    mate, ypeer, xpeer = (d, t + 1 - 2 * c), (1 - d, t), (d, (t + 2) % 4)
    unit0 = pl.multiple_of(d * SKIP, 128)

    def remote(src, dst, sems, i, peer):
        return pltpu.make_async_remote_copy(
            src_ref=src, dst_ref=dst, send_sem=sems.at[sems.shape[0] - 1], recv_sem=sems.at[i],
            device_id=peer, device_id_type=MESH)

    def all_sent(sems, blocks):
        some = xpart.at[pl.ds(0, blocks)]
        pltpu.make_async_copy(some, some, sems.at[sems.shape[0] - 1]).wait()

    def chunk(i):
        pair = (i - 2) // 2
        j = jnp.where(i < 2, i, jnp.where(i < 8, jnp.where(i % 2 == 0, pair + 2, pair), i - 5))
        relayed = jnp.where(i < 8, jnp.where(i < 2, 0, i % 2), 1)
        return 2 * j + jnp.where(relayed == 1, 1 - xi, xi)

    def x_own(k):
        return pltpu.make_async_copy(x.at[:, pl.ds(k * KC, KC)], xs.at[k, pl.ds(0, ROWS)], xsem.at[0])

    def slab(i, which):
        w = (wg, wu)[which]
        rows = pl.ds(pl.multiple_of(chunk(i) * KC, KC), KC)
        s = i % GS
        return pltpu.make_async_copy(w.at[rows, pl.ds(unit0, U)], gu.at[s, which], gsem.at[s])

    def down(n, half):
        s = n % DS
        cols = pl.ds(pl.multiple_of(n * NC + jnp.where(half == 0, c, 1 - c) * HC, HC), HC)
        return pltpu.make_async_copy(
            wd.at[pl.ds(unit0, U), cols], dn.at[s, :, pl.ds(half * HC, HC)], dsem.at[s])

    def load(n):
        down(n, 0).start(priority=1)
        down(n, 1).start(priority=1)

    def other(k, core):
        return xs.at[k, pl.ds(ROWS, ROWS), pl.ds(pl.multiple_of(core * (KC // 2), KC // 2), KC // 2)]

    def mine_x(k):
        return xs.at[k, pl.ds(0, ROWS), pl.ds(pl.multiple_of(c * (KC // 2), KC // 2), KC // 2)]

    def send_y(j):
        return remote(mine_x(2 * j + xi), other(2 * j + xi, c), in_y, j, ypeer)

    def relay_x(j):
        return remote(other(2 * j + xi, c), other(2 * j + xi, c), in_x, j, xpeer)

    def got_x(j):
        return remote(other(2 * j + 1 - xi, c), other(2 * j + 1 - xi, c), in_x, j, xpeer)

    def to_mate(j, relayed):
        k = 2 * j + (1 - xi if relayed else xi)
        return remote(other(k, c), other(k, c), in_m, j + 5 * relayed, mate)

    def from_mate(j, relayed):
        k = 2 * j + (1 - xi if relayed else xi)
        return remote(other(k, 1 - c), other(k, 1 - c), in_m, j + 5 * relayed, mate)

    for k in range(NK):
        x_own(k).start()
    for i in range(GS):
        slab(i, 0).start(priority=1)
        slab(i, 1).start(priority=1)
    barrier = pltpu.get_barrier_semaphore()
    for peer in (mate, ypeer, xpeer):
        pl.semaphore_signal(barrier, inc=1, device_id=peer, device_id_type=MESH)
    acc[...] = jnp.zeros_like(acc)
    with jax.named_scope("bar"):
        pl.semaphore_wait(barrier, 3)
    with jax.named_scope("wxown"):
        pltpu.make_async_copy(x, o, xsem.at[0]).wait()
    for j in range(5):
        send_y(j).start()
    def direct(j):
        with jax.named_scope("wdirect"):
            send_y(j).wait_recv()
        relay_x(j).start()
        to_mate(j, 0).start()

    def relayed(j):
        with jax.named_scope("wrelay"):
            got_x(j).wait_recv()
        to_mate(j, 1).start()

    def whole(j, was_relayed):
        with jax.named_scope("wmate"):
            from_mate(j, was_relayed).wait_recv()

    here = set()

    def arrived(i):
        if i in here:
            return
        here.add(i)
        with jax.named_scope("wslab"):
            pltpu.make_async_copy(gu.at[i % GS], gu.at[i % GS], gsem.at[i % GS]).wait()

    def free(i):
        if i + GS < NK:
            slab(i + GS, 0).start(priority=1)
            slab(i + GS, 1).start(priority=1)

    def multiply(i, rows):
        xk = xs[chunk(i), rows]
        with jax.named_scope("dot1"):
            for which in range(2):
                acc[rows, which * U:(which + 1) * U] += jnp.dot(xk, gu[i % GS, which], preferred_element_type=F32)

    own, others, both = slice(0, ROWS), slice(ROWS, 2 * ROWS), slice(0, 2 * ROWS)
    relayed_ones = {3: 0, 5: 1, 7: 2, 8: 3, 9: 4}
    direct_ones = {0: 0, 1: 1, 2: 2, 4: 3, 6: 4}

    def complete(i):
        if i in relayed_ones:
            whole(relayed_ones[i], 1)
        else:
            whole(direct_ones[i], 0)

    def last(i, rows):
        xk = xs[chunk(i), rows]
        with jax.named_scope("dot1last"):
            for b in range(U // 256):
                gate, up = (
                    acc[rows, w * U + b * 256:w * U + (b + 1) * 256]
                    + jnp.dot(xk, gu[i % GS, w, :, b * 256:(b + 1) * 256], preferred_element_type=F32)
                    for w in range(2))
                h[rows, b * 256:(b + 1) * 256] = (jax.nn.silu(gate) * up).astype(BF16)

        @pl.when(d == 1)
        def _():
            h[rows, 0:2 * U - FF] = jnp.zeros((ROWS, 2 * U - FF), BF16)

    def O(*steps):
        for i in steps:
            arrived(i)
        for i in steps:
            multiply(i, own)

    def X(*steps):
        for i in steps:
            complete(i)
        for i in steps:
            arrived(i)
        for i in steps:
            multiply(i, others)

    def F(*steps):
        for i in steps:
            complete(i)
        for i in steps:
            arrived(i)
        for i in steps:
            multiply(i, both)

    def swap_x(n):
        return remote(xpart.at[n], xgot.at[n], sx, n % RING, mate)

    def swap_o(n):
        return remote(opart.at[n], ogot.at[n], so, n % RING, mate)

    def part(q):
        return pl.ds(q * (ROWS // 2), ROWS // 2)

    def cross_y(n, q):
        return remote(ysend.at[n, part(q)], yrecv.at[n, part(q)], out_y, 2 * (n % RING_Y) + q, ypeer)

    def cross_x(n, q):
        return remote(xsend.at[n, part(q)], xrecv.at[n, part(q)], out_x, 2 * n + q, xpeer)

    def give(n):
        cols = pl.ds(pl.multiple_of(n * NC + c * HC, HC), HC)
        return remote(o.at[:, cols], o.at[:, cols], out_o, 0, mate)

    def loaded(n):
        with jax.named_scope("wdown"):
            pltpu.make_async_copy(dn.at[n % DS], dn.at[n % DS], dsem.at[n % DS]).wait()

    def more(n):
        @pl.when(n + DS < NN)
        def _():
            load(n + DS)

    def product_x(n):
        loaded(n)
        with jax.named_scope("dot2"):
            p = jnp.dot(h[others], dn[n % DS], preferred_element_type=F32)
            xkeep[n] = p[:, :HC]
            xpart[n] = p[:, HC:].astype(BF16)
        swap_x(n).start()

    def product_o(n):
        with jax.named_scope("dot2"):
            p = jnp.dot(h[own], dn[n % DS], preferred_element_type=F32)
            okeep[n] = p[:, :HC]
            opart[n] = p[:, HC:].astype(BF16)
        swap_o(n).start()
        more(n)

    def products(n, m):
        loaded(n)
        with jax.named_scope("dot2b"):
            p = jnp.dot(h[others], dn[n % DS], preferred_element_type=F32)
            r = jnp.dot(h[own], dn[m % DS], preferred_element_type=F32)
            xkeep[n] = p[:, :HC]
            xpart[n] = p[:, HC:].astype(BF16)
            okeep[m] = r[:, :HC]
            opart[m] = r[:, HC:].astype(BF16)
        swap_x(n).start()
        swap_o(m).start()
        more(m)

    def pass_y(n):
        with jax.named_scope("wswap"):
            swap_x(n).wait_recv()
        ysend[n] = (xkeep[n] + xgot[n].astype(F32)).astype(BF16)
        cross_y(n, 0).start()
        cross_y(n, 1).start()

    def pass_x(n, q):
        if q == 0:
            with jax.named_scope("wswapo"):
                swap_o(n).wait_recv()
        with jax.named_scope("wy"):
            cross_y(n, q).wait_recv()
        r = part(q)
        xsend[n, r] = (okeep[n, r] + ogot[n, r].astype(F32) + yrecv[n, r].astype(F32)).astype(BF16)
        cross_x(n, q).start()

    def finish(n):
        with jax.named_scope("wx"):
            cross_x(n, 0).wait_recv()
            cross_x(n, 1).wait_recv()
        cols = pl.ds(pl.multiple_of(n * NC + c * HC, HC), HC)
        o[:, cols] = (xsend[n].astype(F32) + xrecv[n].astype(F32)).astype(BF16)
        give(n).start()

    O(0)
    O(1)
    direct(0)
    O(2)
    direct(1)
    X(0)
    free(0)
    O(3)
    direct(2)
    X(1)
    free(1)
    relayed(0)
    X(2)
    free(2)
    direct(3)
    X(3)
    free(3)
    relayed(1)
    direct(4)
    O(4)
    X(4)
    relayed(2)
    F(5)
    relayed(3)
    F(6)
    load(0)
    relayed(4)
    X(7)
    load(1)
    X(8)
    load(2)
    complete(9)
    arrived(9)
    last(9, others)
    for n in range(3, DS):
        load(n)
    product_x(0)
    product_x(1)
    O(7)
    pass_y(0)
    product_x(2)
    pass_y(1)
    multiply(8, own)
    last(9, own)
    pass_y(2)
    product_o(0)
    products(3, 1)

    @pl.loop(LAG_Y, NN + LAG_X)
    def _(n):
        @pl.when(n < NN + LAG_Y)
        def _():
            pass_x(n - LAG_Y, 0)

        @pl.when(n < NN - 1)
        def _():
            products(n + 1, n - 1)

        @pl.when(jnp.logical_and(n >= NN - 1, n < NN + 1))
        def _():
            product_o(n - 1)

        @pl.when(n < NN)
        def _():
            pass_y(n)

        @pl.when(n < NN + LAG_Y)
        def _():
            pass_x(n - LAG_Y, 1)

        @pl.when(n >= LAG_X)
        def _():
            finish(n - LAG_X)

    with jax.named_scope("wgive"):
        pltpu.make_async_copy(xpart, xpart, out_o.at[0]).wait()

    with jax.named_scope("wend"):
        for sems in (in_y, in_x):
            all_sent(sems, 5)
        for sems in (in_m, sx, so, out_y, out_x, out_o):
            all_sent(sems, NN)


def solution(mesh):
    dma = pltpu.SemaphoreType.DMA
    vmem = pltpu.VMEM

    def step(x, w_gate, w_up, w_down):
        return pl.pallas_call(
            kernel,
            out_shape=pltpu.VMEM((ROWS, D), BF16),
            in_specs=[pl.BlockSpec(memory_space=pl.ANY)] * 4,
            out_specs=pl.BlockSpec(memory_space=pltpu.VMEM),
            scratch_shapes=[
                vmem((NK, 2 * ROWS, KC), BF16),
                vmem((2 * ROWS, 2 * U), F32),
                vmem((2 * ROWS, U), BF16),
                vmem((GS, 2, KC, U), BF16),
                vmem((DS, U, NC), BF16),
                vmem((NN, ROWS, HC), F32),
                vmem((NN, ROWS, HC), F32),
                *[vmem((NN, ROWS, HC), BF16)] * 8,
                dma((1,)),
                dma((GS,)),
                dma((DS,)),
                dma((6,)),
                dma((6,)),
                dma((11,)),
                *[dma((RING + 1,))] * 2,
                dma((2 * RING_Y + 1,)),
                dma((2 * NN + 1,)),
                dma((2,)),
            ],
            compiler_params=pltpu.CompilerParams(
                collective_id=0, has_side_effects=True, vmem_limit_bytes=61 * 2**20),
        )(x, w_gate, w_up, w_down)

    return jax.shard_map(
        step,
        mesh=mesh,
        in_specs=(P("dp", None), P(None, "tp"), P(None, "tp"), P("tp", None)),
        out_specs=P("dp", None),
        check_vma=False,
    )
```

```python
import jax
import jax.numpy as jnp
from jax import lax
from jax.experimental import pallas as pl
from jax.experimental.pallas import tpu as pltpu
from jax.sharding import PartitionSpec as P

MESH = pl.DeviceIdType.MESH
ROWS, D, FF = 128, 5120, 4480
U = 2304
SKIP = FF - U
KC = 512
NK = D // KC
NC = 512
NN = D // NC
HC = NC // 2
NB = NN + 1
GS = 6
DS = 6
LAG_Y, LAG_X = 3, 6
RING, RING_Y = 6, 8
F32, BF16 = jnp.float32, jnp.bfloat16


def kernel(x, wg, wu, wd, o, xs, acc, h, gu, dn, xkeep, okeep, xpart, xgot, opart, ogot, ysend, yrecv, xsend, xrecv,
           xsem, gsem, dsem, in_y, in_x, in_m, sx, so, out_y, out_x, out_o):
    d, t = lax.axis_index("dp"), lax.axis_index("tp")
    xi, c = t // 2, t % 2
    mate, ypeer, xpeer = (d, t + 1 - 2 * c), (1 - d, t), (d, (t + 2) % 4)
    unit0 = pl.multiple_of(d * SKIP, 128)

    def remote(src, dst, sems, i, peer):
        return pltpu.make_async_remote_copy(
            src_ref=src, dst_ref=dst, send_sem=sems.at[sems.shape[0] - 1], recv_sem=sems.at[i],
            device_id=peer, device_id_type=MESH)

    def all_sent(sems, blocks):
        some = xpart.at[pl.ds(0, blocks)]
        pltpu.make_async_copy(some, some, sems.at[sems.shape[0] - 1]).wait()

    def chunk(i):
        pair = (i - 2) // 2
        j = jnp.where(i < 2, i, jnp.where(i < 8, jnp.where(i % 2 == 0, pair + 2, pair), i - 5))
        relayed = jnp.where(i < 8, jnp.where(i < 2, 0, i % 2), 1)
        return 2 * j + jnp.where(relayed == 1, 1 - xi, xi)

    def x_own(k):
        return pltpu.make_async_copy(x.at[:, pl.ds(k * KC, KC)], xs.at[k, pl.ds(0, ROWS)], xsem.at[0])

    def slab(i, which):
        w = (wg, wu)[which]
        rows = pl.ds(pl.multiple_of(chunk(i) * KC, KC), KC)
        s = i % GS
        return pltpu.make_async_copy(w.at[rows, pl.ds(unit0, U)], gu.at[s, which], gsem.at[s])

    def down(n, half):
        s = n % DS
        first = jnp.where(n == NN - 1, half, jnp.where(half == 0, c, 1 - c))
        cols = pl.ds(pl.multiple_of(n * NC + first * HC, HC), HC)
        return pltpu.make_async_copy(
            wd.at[pl.ds(unit0, U), cols], dn.at[s, :, pl.ds(half * HC, HC)], dsem.at[s])

    def load(n):
        down(n, 0).start(priority=1)
        down(n, 1).start(priority=1)

    def other(k, core):
        return xs.at[k, pl.ds(ROWS, ROWS), pl.ds(pl.multiple_of(core * (KC // 2), KC // 2), KC // 2)]

    def mine_x(k):
        return xs.at[k, pl.ds(0, ROWS), pl.ds(pl.multiple_of(c * (KC // 2), KC // 2), KC // 2)]

    def send_y(j):
        return remote(mine_x(2 * j + xi), other(2 * j + xi, c), in_y, j, ypeer)

    def relay_x(j):
        return remote(other(2 * j + xi, c), other(2 * j + xi, c), in_x, j, xpeer)

    def got_x(j):
        return remote(other(2 * j + 1 - xi, c), other(2 * j + 1 - xi, c), in_x, j, xpeer)

    def to_mate(j, relayed):
        k = 2 * j + (1 - xi if relayed else xi)
        return remote(other(k, c), other(k, c), in_m, j + 5 * relayed, mate)

    def from_mate(j, relayed):
        k = 2 * j + (1 - xi if relayed else xi)
        return remote(other(k, 1 - c), other(k, 1 - c), in_m, j + 5 * relayed, mate)

    for k in range(NK):
        x_own(k).start()
    for i in range(GS):
        slab(i, 0).start(priority=1)
        slab(i, 1).start(priority=1)
    barrier = pltpu.get_barrier_semaphore()
    for peer in (mate, ypeer, xpeer):
        pl.semaphore_signal(barrier, inc=1, device_id=peer, device_id_type=MESH)
    acc[...] = jnp.zeros_like(acc)
    with jax.named_scope("bar"):
        pl.semaphore_wait(barrier, 3)
    with jax.named_scope("wxown"):
        pltpu.make_async_copy(x, o, xsem.at[0]).wait()
    for j in range(5):
        send_y(j).start()
    def direct(j):
        with jax.named_scope("wdirect"):
            send_y(j).wait_recv()
        relay_x(j).start()
        to_mate(j, 0).start()

    def relayed(j):
        with jax.named_scope("wrelay"):
            got_x(j).wait_recv()
        to_mate(j, 1).start()

    def whole(j, was_relayed):
        with jax.named_scope("wmate"):
            from_mate(j, was_relayed).wait_recv()

    here = set()

    def arrived(i):
        if i in here:
            return
        here.add(i)
        with jax.named_scope("wslab"):
            pltpu.make_async_copy(gu.at[i % GS], gu.at[i % GS], gsem.at[i % GS]).wait()

    def free(i):
        if i + GS < NK:
            slab(i + GS, 0).start(priority=1)
            slab(i + GS, 1).start(priority=1)

    def multiply(i, rows):
        xk = xs[chunk(i), rows]
        with jax.named_scope("dot1"):
            for which in range(2):
                acc[rows, which * U:(which + 1) * U] += jnp.dot(xk, gu[i % GS, which], preferred_element_type=F32)

    own, others, both = slice(0, ROWS), slice(ROWS, 2 * ROWS), slice(0, 2 * ROWS)
    relayed_ones = {3: 0, 5: 1, 7: 2, 8: 3, 9: 4}
    direct_ones = {0: 0, 1: 1, 2: 2, 4: 3, 6: 4}

    def complete(i):
        if i in relayed_ones:
            whole(relayed_ones[i], 1)
        else:
            whole(direct_ones[i], 0)

    def multiply_part(i, rows, core):
        cut = pl.ds(pl.multiple_of(core * (KC // 2), KC // 2), KC // 2)
        xk = xs[chunk(i), rows, cut]
        with jax.named_scope("dot1p"):
            for which in range(2):
                acc[rows, which * U:(which + 1) * U] += jnp.dot(
                    xk, gu[i % GS, which, cut], preferred_element_type=F32)

    def last(i, rows):
        xk = xs[chunk(i), rows]
        with jax.named_scope("dot1last"):
            for b in range(U // 256):
                gate, up = (
                    acc[rows, w * U + b * 256:w * U + (b + 1) * 256]
                    + jnp.dot(xk, gu[i % GS, w, :, b * 256:(b + 1) * 256], preferred_element_type=F32)
                    for w in range(2))
                h[rows, b * 256:(b + 1) * 256] = (jax.nn.silu(gate) * up).astype(BF16)

        @pl.when(d == 1)
        def _():
            h[rows, 0:2 * U - FF] = jnp.zeros((ROWS, 2 * U - FF), BF16)

    def O(*steps):
        for i in steps:
            arrived(i)
        for i in steps:
            multiply(i, own)

    def X(*steps):
        for i in steps:
            complete(i)
        for i in steps:
            arrived(i)
        for i in steps:
            multiply(i, others)

    def F(*steps):
        for i in steps:
            complete(i)
        for i in steps:
            arrived(i)
        for i in steps:
            multiply(i, both)

    def swap_x(n):
        return remote(xpart.at[n], xgot.at[n], sx, n % RING, mate)

    def swap_o(n):
        return remote(opart.at[n], ogot.at[n], so, n % RING, mate)

    def part(q):
        return pl.ds(q * (ROWS // 2), ROWS // 2)

    def cross_y(n, q):
        return remote(ysend.at[n, part(q)], yrecv.at[n, part(q)], out_y, 2 * (n % RING_Y) + q, ypeer)

    def cross_x(n, q):
        return remote(xsend.at[n, part(q)], xrecv.at[n, part(q)], out_x, 2 * n + q, xpeer)

    def columns(n):
        start = jnp.where(n < NN - 1, n * NC + c * HC, (NN - 1) * NC + (n - NN + 1) * HC)
        return pl.ds(pl.multiple_of(start, HC), HC)

    def give(n):
        return remote(o.at[:, columns(n)], o.at[:, columns(n)], out_o, 0, mate)

    def loaded(n):
        with jax.named_scope("wdown"):
            pltpu.make_async_copy(dn.at[n % DS], dn.at[n % DS], dsem.at[n % DS]).wait()

    def more(n):
        @pl.when(n + DS < NN)
        def _():
            load(n + DS)

    def product_x(n):
        loaded(n)
        with jax.named_scope("dot2"):
            p = jnp.dot(h[others], dn[n % DS], preferred_element_type=F32)
            xkeep[n] = p[:, :HC]
            xpart[n] = p[:, HC:].astype(BF16)
        swap_x(n).start()

    def product_o(n):
        with jax.named_scope("dot2"):
            p = jnp.dot(h[own], dn[n % DS], preferred_element_type=F32)
            okeep[n] = p[:, :HC]
            opart[n] = p[:, HC:].astype(BF16)
        swap_o(n).start()
        more(n)

    def products(n, m):
        loaded(n)
        with jax.named_scope("dot2b"):
            p = jnp.dot(h[others], dn[n % DS], preferred_element_type=F32)
            r = jnp.dot(h[own], dn[m % DS], preferred_element_type=F32)
            xkeep[n] = p[:, :HC]
            xpart[n] = p[:, HC:].astype(BF16)
            okeep[m] = r[:, :HC]
            opart[m] = r[:, HC:].astype(BF16)
        swap_x(n).start()
        swap_o(m).start()
        more(m)

    def last_products(m):
        loaded(NN - 1)
        p = jnp.dot(h[others], dn[(NN - 1) % DS], preferred_element_type=F32)
        r = jnp.dot(h[own], dn[m % DS], preferred_element_type=F32)
        for i in range(2):
            xkeep[NN - 1 + i] = p[:, i * HC:(i + 1) * HC]
            xpart[NN - 1 + i] = p[:, i * HC:(i + 1) * HC].astype(BF16)
        okeep[m] = r[:, :HC]
        opart[m] = r[:, HC:].astype(BF16)
        swap_o(m).start()

        @pl.when(c == 0)
        def _():
            swap_x(NN - 1).start()
            swap_x(NN).start()

    def last_own_products(m):
        r = jnp.dot(h[own], dn[m % DS], preferred_element_type=F32)
        p = jnp.dot(h[own], dn[(NN - 1) % DS], preferred_element_type=F32)
        okeep[m] = r[:, :HC]
        opart[m] = r[:, HC:].astype(BF16)
        for i in range(2):
            okeep[NN - 1 + i] = p[:, i * HC:(i + 1) * HC]
            opart[NN - 1 + i] = p[:, i * HC:(i + 1) * HC].astype(BF16)
        swap_o(m).start()

        @pl.when(c == 0)
        def _():
            swap_o(NN - 1).start()
            swap_o(NN).start()

    def pass_y(n):
        with jax.named_scope("wswap"):
            swap_x(n).wait_recv()
        ysend[n] = (xkeep[n] + xgot[n].astype(F32)).astype(BF16)
        cross_y(n, 0).start()
        cross_y(n, 1).start()

    def pass_x(n, q):
        if q == 0:
            with jax.named_scope("wswapo"):
                swap_o(n).wait_recv()
        with jax.named_scope("wy"):
            cross_y(n, q).wait_recv()
        r = part(q)
        xsend[n, r] = (okeep[n, r] + ogot[n, r].astype(F32) + yrecv[n, r].astype(F32)).astype(BF16)
        cross_x(n, q).start()

    def finish(n):
        with jax.named_scope("wx"):
            cross_x(n, 0).wait_recv()
            cross_x(n, 1).wait_recv()
        o[:, columns(n)] = (xsend[n].astype(F32) + xrecv[n].astype(F32)).astype(BF16)
        give(n).start()

    O(0)
    O(1)
    direct(0)
    multiply_part(0, others, c)
    O(2)
    direct(1)
    complete(0)
    multiply_part(0, others, 1 - c)
    free(0)
    O(3)
    direct(2)
    X(1)
    free(1)
    relayed(0)
    X(2)
    free(2)
    direct(3)
    X(3)
    free(3)
    relayed(1)
    direct(4)
    O(4)
    X(4)
    relayed(2)
    F(5)
    relayed(3)
    F(6)
    load(0)
    relayed(4)
    load(1)
    complete(7)
    complete(8)
    arrived(7)
    arrived(8)
    multiply(7, others)
    multiply(8, others)
    load(2)
    complete(9)
    arrived(9)
    last(9, others)
    for n in range(3, DS):
        load(n)
    product_x(0)
    product_x(1)
    O(7)
    pass_y(0)
    product_x(2)
    pass_y(1)
    multiply(8, own)
    last(9, own)
    product_o(0)
    pass_y(2)
    products(3, 1)

    @pl.loop(LAG_Y, NN - 2)
    def _(n):
        pass_x(n - LAG_Y, 0)
        products(n + 1, n - 1)
        pass_y(n)
        pass_x(n - LAG_Y, 1)

        @pl.when(n >= LAG_X)
        def _():
            finish(n - LAG_X)

    pass_x(NN - 5, 0)
    last_products(NN - 3)
    pass_y(NN - 2)
    pass_x(NN - 5, 1)
    finish(NN - 8)
    pass_x(NN - 4, 0)
    last_own_products(NN - 2)
    pass_x(NN - 4, 1)

    @pl.when(c == 1)
    def _():
        pass_y(NN - 1)
        pass_y(NN)

    finish(NN - 7)
    for n in (NN - 3, NN - 2):
        pass_x(n, 0)
        pass_x(n, 1)
        finish(n - 3)

    @pl.when(c == 1)
    def _():
        for n in (NN - 1, NN):
            pass_x(n, 0)
            pass_x(n, 1)

    for n in (NN - 4, NN - 3, NN - 2):
        finish(n)

    @pl.when(c == 1)
    def _():
        finish(NN - 1)
        finish(NN)

    for sems in (in_y, in_x):
        all_sent(sems, 5)
    all_sent(in_m, 10)
    for core in range(2):
        mine, gone = (NN - 1, NB) if core == 0 else (NB, NN - 1)

        @pl.when(c == core)
        def _():
            with jax.named_scope("wgive"):
                theirs = xpart.at[pl.ds(0, gone)]
                pltpu.make_async_copy(theirs, theirs, out_o.at[0]).wait()
            for sems in (sx, so):
                all_sent(sems, gone)
            for sems in (out_y, out_x, out_o):
                all_sent(sems, mine)


def solution(mesh):
    dma = pltpu.SemaphoreType.DMA
    vmem = pltpu.VMEM

    def step(x, w_gate, w_up, w_down):
        return pl.pallas_call(
            kernel,
            out_shape=pltpu.VMEM((ROWS, D), BF16),
            in_specs=[pl.BlockSpec(memory_space=pl.ANY)] * 4,
            out_specs=pl.BlockSpec(memory_space=pltpu.VMEM),
            scratch_shapes=[
                vmem((NK, 2 * ROWS, KC), BF16),
                vmem((2 * ROWS, 2 * U), F32),
                vmem((2 * ROWS, U), BF16),
                vmem((GS, 2, KC, U), BF16),
                vmem((DS, U, NC), BF16),
                *[vmem((NB, ROWS, HC), F32)] * 2,
                *[vmem((NB, ROWS, HC), BF16)] * 8,
                dma((1,)),
                dma((GS,)),
                dma((DS,)),
                dma((6,)),
                dma((6,)),
                dma((11,)),
                *[dma((RING + 1,))] * 2,
                dma((2 * RING_Y + 1,)),
                dma((2 * NB + 1,)),
                dma((2,)),
            ],
            compiler_params=pltpu.CompilerParams(
                collective_id=0, has_side_effects=True, vmem_limit_bytes=61 * 2**20),
        )(x, w_gate, w_up, w_down)

    return jax.shard_map(
        step,
        mesh=mesh,
        in_specs=(P("dp", None), P(None, "tp"), P(None, "tp"), P("tp", None)),
        out_specs=P("dp", None),
        check_vma=False,
    )
```

```python
import jax
import jax.numpy as jnp
from jax import lax
from jax.experimental import pallas as pl
from jax.experimental.pallas import tpu as pltpu
from jax.sharding import PartitionSpec as P

MESH = pl.DeviceIdType.MESH
ROWS, D, FF = 128, 5120, 4480
U = 2304
SKIP = FF - U
KC = 512
NK = D // KC
NC = 512
NN = D // NC
HC = NC // 2
NB = NN + 1
GS = 6
DS = 6
LAG_Y, LAG_X = 3, 6
RING, RING_Y = 6, 8
F32, BF16 = jnp.float32, jnp.bfloat16


def kernel(x, wg, wu, wd, o, xs, acc, h, gu, dn, xkeep, okeep, xpart, xgot, opart, ogot, ysend, yrecv, xsend, xrecv,
           xsem, gsem, dsem, in_y, in_x, in_m, sx, so, out_y, out_x, out_o):
    d, t = lax.axis_index("dp"), lax.axis_index("tp")
    xi, c = t // 2, t % 2
    mate, ypeer, xpeer = (d, t + 1 - 2 * c), (1 - d, t), (d, (t + 2) % 4)
    unit0 = pl.multiple_of(d * SKIP, 128)

    def remote(src, dst, sems, i, peer):
        return pltpu.make_async_remote_copy(
            src_ref=src, dst_ref=dst, send_sem=sems.at[sems.shape[0] - 1], recv_sem=sems.at[i],
            device_id=peer, device_id_type=MESH)

    def all_sent(sems, blocks):
        some = xpart.at[pl.ds(0, blocks)]
        pltpu.make_async_copy(some, some, sems.at[sems.shape[0] - 1]).wait()

    def chunk(i):
        pair = (i - 2) // 2
        j = jnp.where(i < 2, i, jnp.where(i < 8, jnp.where(i % 2 == 0, pair + 2, pair), i - 5))
        relayed = jnp.where(i < 8, jnp.where(i < 2, 0, i % 2), 1)
        return 2 * j + jnp.where(relayed == 1, 1 - xi, xi)

    def x_own(k):
        return pltpu.make_async_copy(x.at[:, pl.ds(k * KC, KC)], xs.at[k, pl.ds(0, ROWS)], xsem.at[0])

    def slab(i, which):
        w = (wg, wu)[which]
        rows = pl.ds(pl.multiple_of(chunk(i) * KC, KC), KC)
        s = i % GS
        return pltpu.make_async_copy(w.at[rows, pl.ds(unit0, U)], gu.at[s, which], gsem.at[s])

    def down(n, half):
        s = n % DS
        first = jnp.where(n == NN - 1, half, jnp.where(half == 0, c, 1 - c))
        cols = pl.ds(pl.multiple_of(n * NC + first * HC, HC), HC)
        return pltpu.make_async_copy(
            wd.at[pl.ds(unit0, U), cols], dn.at[s, :, pl.ds(half * HC, HC)], dsem.at[s])

    def load(n):
        down(n, 0).start(priority=1)
        down(n, 1).start(priority=1)

    def other(k, core):
        return xs.at[k, pl.ds(ROWS, ROWS), pl.ds(pl.multiple_of(core * (KC // 2), KC // 2), KC // 2)]

    def mine_x(k):
        return xs.at[k, pl.ds(0, ROWS), pl.ds(pl.multiple_of(c * (KC // 2), KC // 2), KC // 2)]

    def send_y(j):
        return remote(mine_x(2 * j + xi), other(2 * j + xi, c), in_y, j, ypeer)

    def relay_x(j):
        return remote(other(2 * j + xi, c), other(2 * j + xi, c), in_x, j, xpeer)

    def got_x(j):
        return remote(other(2 * j + 1 - xi, c), other(2 * j + 1 - xi, c), in_x, j, xpeer)

    def to_mate(j, relayed):
        k = 2 * j + (1 - xi if relayed else xi)
        return remote(other(k, c), other(k, c), in_m, j + 5 * relayed, mate)

    def from_mate(j, relayed):
        k = 2 * j + (1 - xi if relayed else xi)
        return remote(other(k, 1 - c), other(k, 1 - c), in_m, j + 5 * relayed, mate)

    for k in range(NK):
        x_own(k).start()
    for i in range(GS):
        slab(i, 0).start(priority=1)
        slab(i, 1).start(priority=1)
    barrier = pltpu.get_barrier_semaphore()
    for peer in (mate, ypeer, xpeer):
        pl.semaphore_signal(barrier, inc=1, device_id=peer, device_id_type=MESH)
    acc[...] = jnp.zeros_like(acc)
    with jax.named_scope("bar"):
        pl.semaphore_wait(barrier, 3)
    with jax.named_scope("wxown"):
        pltpu.make_async_copy(x, o, xsem.at[0]).wait()
    for j in range(5):
        send_y(j).start()
    def direct(j):
        with jax.named_scope("wdirect"):
            send_y(j).wait_recv()
        relay_x(j).start()
        to_mate(j, 0).start()

    def relayed(j):
        with jax.named_scope("wrelay"):
            got_x(j).wait_recv()
        to_mate(j, 1).start()

    def whole(j, was_relayed):
        with jax.named_scope("wmate"):
            from_mate(j, was_relayed).wait_recv()

    here = set()

    def arrived(i):
        if i in here:
            return
        here.add(i)
        with jax.named_scope("wslab"):
            pltpu.make_async_copy(gu.at[i % GS], gu.at[i % GS], gsem.at[i % GS]).wait()

    def free(i):
        if i + GS < NK:
            slab(i + GS, 0).start(priority=1)
            slab(i + GS, 1).start(priority=1)

    def multiply(i, rows):
        xk = xs[chunk(i), rows]
        with jax.named_scope("dot1"):
            for which in range(2):
                acc[rows, which * U:(which + 1) * U] += jnp.dot(xk, gu[i % GS, which], preferred_element_type=F32)

    own, others, both = slice(0, ROWS), slice(ROWS, 2 * ROWS), slice(0, 2 * ROWS)
    relayed_ones = {3: 0, 5: 1, 7: 2, 8: 3, 9: 4}
    direct_ones = {0: 0, 1: 1, 2: 2, 4: 3, 6: 4}

    def complete(i):
        if i in relayed_ones:
            whole(relayed_ones[i], 1)
        else:
            whole(direct_ones[i], 0)

    def multiply_part(i, rows, core):
        cut = pl.ds(pl.multiple_of(core * (KC // 2), KC // 2), KC // 2)
        xk = xs[chunk(i), rows, cut]
        with jax.named_scope("dot1p"):
            for which in range(2):
                acc[rows, which * U:(which + 1) * U] += jnp.dot(
                    xk, gu[i % GS, which, cut], preferred_element_type=F32)

    def last(i, rows):
        xk = xs[chunk(i), rows]
        with jax.named_scope("dot1last"):
            for b in range(U // 256):
                gate, up = (
                    acc[rows, w * U + b * 256:w * U + (b + 1) * 256]
                    + jnp.dot(xk, gu[i % GS, w, :, b * 256:(b + 1) * 256], preferred_element_type=F32)
                    for w in range(2))
                h[rows, b * 256:(b + 1) * 256] = (jax.nn.silu(gate) * up).astype(BF16)

        @pl.when(d == 1)
        def _():
            h[rows, 0:2 * U - FF] = jnp.zeros((ROWS, 2 * U - FF), BF16)

    def O(*steps):
        for i in steps:
            arrived(i)
        for i in steps:
            multiply(i, own)

    def X(*steps):
        for i in steps:
            complete(i)
        for i in steps:
            arrived(i)
        for i in steps:
            multiply(i, others)

    def F(*steps):
        for i in steps:
            complete(i)
        for i in steps:
            arrived(i)
        for i in steps:
            multiply(i, both)

    def swap_x(n):
        return remote(xpart.at[n], xgot.at[n], sx, n % RING, mate)

    def swap_o(n):
        return remote(opart.at[n], ogot.at[n], so, n % RING, mate)

    def part(q):
        return pl.ds(q * (ROWS // 2), ROWS // 2)

    def cross_y(n, q):
        return remote(ysend.at[n, part(q)], yrecv.at[n, part(q)], out_y, 2 * (n % RING_Y) + q, ypeer)

    def cross_x(n, q):
        return remote(xsend.at[n, part(q)], xrecv.at[n, part(q)], out_x, 2 * n + q, xpeer)

    def columns(n):
        start = jnp.where(n < NN - 1, n * NC + c * HC, (NN - 1) * NC + (n - NN + 1) * HC)
        return pl.ds(pl.multiple_of(start, HC), HC)

    def give(n):
        return remote(o.at[:, columns(n)], o.at[:, columns(n)], out_o, 0, mate)

    def loaded(n):
        with jax.named_scope("wdown"):
            pltpu.make_async_copy(dn.at[n % DS], dn.at[n % DS], dsem.at[n % DS]).wait()

    def more(n):
        @pl.when(n + DS < NN)
        def _():
            load(n + DS)

    def product_x(n, here=False):
        if not here:
            loaded(n)
        with jax.named_scope("dot2"):
            p = jnp.dot(h[others], dn[n % DS], preferred_element_type=F32)
            xkeep[n] = p[:, :HC]
            xpart[n] = p[:, HC:].astype(BF16)
        swap_x(n).start()

    def product_o(n):
        with jax.named_scope("dot2"):
            p = jnp.dot(h[own], dn[n % DS], preferred_element_type=F32)
            okeep[n] = p[:, :HC]
            opart[n] = p[:, HC:].astype(BF16)
        swap_o(n).start()
        more(n)

    def products(n, m):
        loaded(n)
        with jax.named_scope("dot2b"):
            p = jnp.dot(h[others], dn[n % DS], preferred_element_type=F32)
            r = jnp.dot(h[own], dn[m % DS], preferred_element_type=F32)
            xkeep[n] = p[:, :HC]
            xpart[n] = p[:, HC:].astype(BF16)
            okeep[m] = r[:, :HC]
            opart[m] = r[:, HC:].astype(BF16)
        swap_x(n).start()
        swap_o(m).start()
        more(m)

    def last_products(m):
        loaded(NN - 1)
        p = jnp.dot(h[others], dn[(NN - 1) % DS], preferred_element_type=F32)
        r = jnp.dot(h[own], dn[m % DS], preferred_element_type=F32)
        for i in range(2):
            xkeep[NN - 1 + i] = p[:, i * HC:(i + 1) * HC]
            xpart[NN - 1 + i] = p[:, i * HC:(i + 1) * HC].astype(BF16)
        okeep[m] = r[:, :HC]
        opart[m] = r[:, HC:].astype(BF16)
        swap_o(m).start()

        @pl.when(c == 0)
        def _():
            swap_x(NN - 1).start()
            swap_x(NN).start()

    def last_own_products(m):
        r = jnp.dot(h[own], dn[m % DS], preferred_element_type=F32)
        p = jnp.dot(h[own], dn[(NN - 1) % DS], preferred_element_type=F32)
        okeep[m] = r[:, :HC]
        opart[m] = r[:, HC:].astype(BF16)
        for i in range(2):
            okeep[NN - 1 + i] = p[:, i * HC:(i + 1) * HC]
            opart[NN - 1 + i] = p[:, i * HC:(i + 1) * HC].astype(BF16)
        swap_o(m).start()

        @pl.when(c == 0)
        def _():
            swap_o(NN - 1).start()
            swap_o(NN).start()

    def pass_y(n):
        with jax.named_scope("wswap"):
            swap_x(n).wait_recv()
        ysend[n] = (xkeep[n] + xgot[n].astype(F32)).astype(BF16)
        cross_y(n, 0).start()
        cross_y(n, 1).start()

    def pass_x(n, q):
        if q == 0:
            with jax.named_scope("wswapo"):
                swap_o(n).wait_recv()
        with jax.named_scope("wy"):
            cross_y(n, q).wait_recv()
        r = part(q)
        xsend[n, r] = (okeep[n, r] + ogot[n, r].astype(F32) + yrecv[n, r].astype(F32)).astype(BF16)
        cross_x(n, q).start()

    def finish(n):
        with jax.named_scope("wx"):
            cross_x(n, 0).wait_recv()
            cross_x(n, 1).wait_recv()
        o[:, columns(n)] = (xsend[n].astype(F32) + xrecv[n].astype(F32)).astype(BF16)
        give(n).start()

    O(0)
    O(1)
    direct(0)
    multiply_part(0, others, c)
    O(2)
    direct(1)
    complete(0)
    multiply_part(0, others, 1 - c)
    free(0)
    O(3)
    direct(2)
    X(1)
    free(1)
    relayed(0)
    X(2)
    free(2)
    direct(3)
    X(3)
    free(3)
    relayed(1)
    direct(4)
    O(4)
    X(4)
    relayed(2)
    F(5)
    relayed(3)
    F(6)
    load(0)
    relayed(4)
    load(1)
    complete(7)
    complete(8)
    arrived(7)
    arrived(8)
    multiply(7, others)
    multiply(8, others)
    load(2)
    complete(9)
    arrived(9)
    last(9, others)
    for n in range(3, DS):
        load(n)
    product_x(0)
    product_x(1)
    loaded(2)
    multiply(7, own)
    product_x(2, True)
    pass_y(0)
    pass_y(1)
    multiply(8, own)
    last(9, own)
    product_o(0)
    pass_y(2)
    products(3, 1)

    @pl.loop(LAG_Y, NN - 2)
    def _(n):
        pass_x(n - LAG_Y, 0)
        products(n + 1, n - 1)
        pass_y(n)
        pass_x(n - LAG_Y, 1)

        @pl.when(n >= LAG_X)
        def _():
            finish(n - LAG_X)

    pass_x(NN - 5, 0)
    last_products(NN - 3)
    pass_y(NN - 2)
    pass_x(NN - 5, 1)
    finish(NN - 8)
    pass_x(NN - 4, 0)
    last_own_products(NN - 2)
    pass_x(NN - 4, 1)

    @pl.when(c == 1)
    def _():
        pass_y(NN - 1)
        pass_y(NN)

    finish(NN - 7)
    for n in (NN - 3, NN - 2):
        pass_x(n, 0)
        pass_x(n, 1)
        finish(n - 3)

    @pl.when(c == 1)
    def _():
        for n in (NN - 1, NN):
            pass_x(n, 0)
            pass_x(n, 1)

    for n in (NN - 4, NN - 3, NN - 2):
        finish(n)

    @pl.when(c == 1)
    def _():
        finish(NN - 1)
        finish(NN)

    for sems in (in_y, in_x):
        all_sent(sems, 5)
    all_sent(in_m, 10)
    for core in range(2):
        mine, gone = (NN - 1, NB) if core == 0 else (NB, NN - 1)

        @pl.when(c == core)
        def _():
            with jax.named_scope("wgive"):
                theirs = xpart.at[pl.ds(0, gone)]
                pltpu.make_async_copy(theirs, theirs, out_o.at[0]).wait()
            for sems in (sx, so):
                all_sent(sems, gone)
            for sems in (out_y, out_x, out_o):
                all_sent(sems, mine)


def solution(mesh):
    dma = pltpu.SemaphoreType.DMA
    vmem = pltpu.VMEM

    def step(x, w_gate, w_up, w_down):
        return pl.pallas_call(
            kernel,
            out_shape=pltpu.VMEM((ROWS, D), BF16),
            in_specs=[pl.BlockSpec(memory_space=pl.ANY)] * 4,
            out_specs=pl.BlockSpec(memory_space=pltpu.VMEM),
            scratch_shapes=[
                vmem((NK, 2 * ROWS, KC), BF16),
                vmem((2 * ROWS, 2 * U), F32),
                vmem((2 * ROWS, U), BF16),
                vmem((GS, 2, KC, U), BF16),
                vmem((DS, U, NC), BF16),
                *[vmem((NB, ROWS, HC), F32)] * 2,
                *[vmem((NB, ROWS, HC), BF16)] * 8,
                dma((1,)),
                dma((GS,)),
                dma((DS,)),
                dma((6,)),
                dma((6,)),
                dma((11,)),
                *[dma((RING + 1,))] * 2,
                dma((2 * RING_Y + 1,)),
                dma((2 * NB + 1,)),
                dma((2,)),
            ],
            compiler_params=pltpu.CompilerParams(
                collective_id=0, has_side_effects=True, vmem_limit_bytes=61 * 2**20),
        )(x, w_gate, w_up, w_down)

    return jax.shard_map(
        step,
        mesh=mesh,
        in_specs=(P("dp", None), P(None, "tp"), P(None, "tp"), P("tp", None)),
        out_specs=P("dp", None),
        check_vma=False,
    )
```

```python
import jax
import jax.numpy as jnp
from jax import lax
from jax.experimental import pallas as pl
from jax.experimental.pallas import tpu as pltpu
from jax.sharding import PartitionSpec as P

MESH = pl.DeviceIdType.MESH
ROWS, D, FF = 128, 5120, 4480
U = 2304
SKIP = FF - U
KC = 512
NK = D // KC
NC = 512
NN = D // NC
HC = NC // 2
NB = NN + 1
GS = 6
DS = 6
LAG_Y, LAG_X = 3, 6
RING, RING_Y, RING_X = 6, 8, 9
F32, BF16 = jnp.float32, jnp.bfloat16


def kernel(x, wg, wu, wd, o, xs, acc, h, gu, dn, xkeep, okeep, xpart, xgot, opart, ogot, ysend, yrecv, xsend, xrecv,
           xsem, gsem, dsem, in_y, in_x, in_m, sx, so, out_y, out_x, out_o, sent):
    d, t = lax.axis_index("dp"), lax.axis_index("tp")
    xi, c = t // 2, t % 2
    mate, ypeer, xpeer = (d, t + 1 - 2 * c), (1 - d, t), (d, (t + 2) % 4)
    unit0 = pl.multiple_of(d * SKIP, 128)

    def remote(src, dst, sems, i, peer):
        return pltpu.make_async_remote_copy(
            src_ref=src, dst_ref=dst, send_sem=sent.at[0], recv_sem=sems.at[i],
            device_id=peer, device_id_type=MESH)

    def all_sent(blocks):
        some = dn.at[pl.ds(0, 2), pl.ds(0, blocks * ROWS * HC // (2 * NC))]
        pltpu.make_async_copy(some, some, sent.at[0]).wait()

    def chunk(i):
        pair = (i - 2) // 2
        j = jnp.where(i < 2, i, jnp.where(i < 8, jnp.where(i % 2 == 0, pair + 2, pair), i - 5))
        relayed = jnp.where(i < 8, jnp.where(i < 2, 0, i % 2), 1)
        return 2 * j + jnp.where(relayed == 1, 1 - xi, xi)

    def x_own(k):
        return pltpu.make_async_copy(x.at[:, pl.ds(k * KC, KC)], xs.at[k, pl.ds(0, ROWS)], xsem.at[0])

    def slab(i, which):
        w = (wg, wu)[which]
        rows = pl.ds(pl.multiple_of(chunk(i) * KC, KC), KC)
        s = i % GS
        return pltpu.make_async_copy(w.at[rows, pl.ds(unit0, U)], gu.at[s, which], gsem.at[s])

    def down(n, half):
        s = n % DS
        first = jnp.where(n == NN - 1, half, jnp.where(half == 0, c, 1 - c))
        cols = pl.ds(pl.multiple_of(n * NC + first * HC, HC), HC)
        return pltpu.make_async_copy(
            wd.at[pl.ds(unit0, U), cols], dn.at[s, :, pl.ds(half * HC, HC)], dsem.at[s])

    def load(n):
        down(n, 0).start(priority=1)
        down(n, 1).start(priority=1)

    def other(k, core):
        return xs.at[k, pl.ds(ROWS, ROWS), pl.ds(pl.multiple_of(core * (KC // 2), KC // 2), KC // 2)]

    def mine_x(k):
        return xs.at[k, pl.ds(0, ROWS), pl.ds(pl.multiple_of(c * (KC // 2), KC // 2), KC // 2)]

    def send_y(j):
        return remote(mine_x(2 * j + xi), other(2 * j + xi, c), in_y, j, ypeer)

    def relay_x(j):
        return remote(other(2 * j + xi, c), other(2 * j + xi, c), in_x, j, xpeer)

    def got_x(j):
        return remote(other(2 * j + 1 - xi, c), other(2 * j + 1 - xi, c), in_x, j, xpeer)

    def to_mate(j, relayed):
        k = 2 * j + (1 - xi if relayed else xi)
        return remote(other(k, c), other(k, c), in_m, j + 5 * relayed, mate)

    def from_mate(j, relayed):
        k = 2 * j + (1 - xi if relayed else xi)
        return remote(other(k, 1 - c), other(k, 1 - c), in_m, j + 5 * relayed, mate)

    for k in range(NK):
        x_own(k).start()
    for i in range(GS):
        slab(i, 0).start(priority=1)
        slab(i, 1).start(priority=1)
    barrier = pltpu.get_barrier_semaphore()
    for peer in (mate, ypeer, xpeer):
        pl.semaphore_signal(barrier, inc=1, device_id=peer, device_id_type=MESH)
    acc[...] = jnp.zeros_like(acc)
    with jax.named_scope("bar"):
        pl.semaphore_wait(barrier, 3)
    with jax.named_scope("wxown"):
        pltpu.make_async_copy(x, o, xsem.at[0]).wait()
    for j in range(5):
        send_y(j).start()
    def direct(j):
        with jax.named_scope("wdirect"):
            send_y(j).wait_recv()
        relay_x(j).start()
        to_mate(j, 0).start()

    def relayed(j):
        with jax.named_scope("wrelay"):
            got_x(j).wait_recv()
        to_mate(j, 1).start()

    def whole(j, was_relayed):
        with jax.named_scope("wmate"):
            from_mate(j, was_relayed).wait_recv()

    here = set()

    def arrived(i):
        if i in here:
            return
        here.add(i)
        with jax.named_scope("wslab"):
            pltpu.make_async_copy(gu.at[i % GS], gu.at[i % GS], gsem.at[i % GS]).wait()

    def free(i):
        if i + GS < NK:
            slab(i + GS, 0).start(priority=1)
            slab(i + GS, 1).start(priority=1)

    def multiply(i, rows):
        xk = xs[chunk(i), rows]
        with jax.named_scope("dot1"):
            for which in range(2):
                acc[rows, which * U:(which + 1) * U] += jnp.dot(xk, gu[i % GS, which], preferred_element_type=F32)

    own, others, both = slice(0, ROWS), slice(ROWS, 2 * ROWS), slice(0, 2 * ROWS)
    relayed_ones = {3: 0, 5: 1, 7: 2, 8: 3, 9: 4}
    direct_ones = {0: 0, 1: 1, 2: 2, 4: 3, 6: 4}

    def complete(i):
        if i in relayed_ones:
            whole(relayed_ones[i], 1)
        else:
            whole(direct_ones[i], 0)

    def multiply_part(i, rows, core):
        cut = pl.ds(pl.multiple_of(core * (KC // 2), KC // 2), KC // 2)
        xk = xs[chunk(i), rows, cut]
        with jax.named_scope("dot1p"):
            for which in range(2):
                acc[rows, which * U:(which + 1) * U] += jnp.dot(
                    xk, gu[i % GS, which, cut], preferred_element_type=F32)

    def last(i, rows):
        xk = xs[chunk(i), rows]
        with jax.named_scope("dot1last"):
            for b in range(U // 256):
                gate, up = (
                    acc[rows, w * U + b * 256:w * U + (b + 1) * 256]
                    + jnp.dot(xk, gu[i % GS, w, :, b * 256:(b + 1) * 256], preferred_element_type=F32)
                    for w in range(2))
                h[rows, b * 256:(b + 1) * 256] = (jax.nn.silu(gate) * up).astype(BF16)

        @pl.when(d == 1)
        def _():
            h[rows, 0:2 * U - FF] = jnp.zeros((ROWS, 2 * U - FF), BF16)

    def O(*steps):
        for i in steps:
            arrived(i)
        for i in steps:
            multiply(i, own)

    def X(*steps):
        for i in steps:
            complete(i)
        for i in steps:
            arrived(i)
        for i in steps:
            multiply(i, others)

    def F(*steps):
        for i in steps:
            complete(i)
        for i in steps:
            arrived(i)
        for i in steps:
            multiply(i, both)

    def swap_x(n):
        return remote(xpart.at[n], xgot.at[n], sx, n % RING, mate)

    def swap_o(n):
        return remote(opart.at[n], ogot.at[n], so, n % RING, mate)

    def part(q):
        return pl.ds(q * (ROWS // 2), ROWS // 2)

    def cross_y(n, q):
        return remote(ysend.at[n, part(q)], yrecv.at[n, part(q)], out_y, 2 * (n % RING_Y) + q, ypeer)

    def cross_x(n, q):
        return remote(xsend.at[n, part(q)], xrecv.at[n, part(q)], out_x, 2 * (n % RING_X) + q, xpeer)

    def columns(n):
        start = jnp.where(n < NN - 1, n * NC + c * HC, (NN - 1) * NC + (n - NN + 1) * HC)
        return pl.ds(pl.multiple_of(start, HC), HC)

    def give(n):
        return remote(o.at[:, columns(n)], o.at[:, columns(n)], out_o, 0, mate)

    def loaded(n):
        with jax.named_scope("wdown"):
            pltpu.make_async_copy(dn.at[n % DS], dn.at[n % DS], dsem.at[n % DS]).wait()

    def more(n):
        @pl.when(n + DS < NN)
        def _():
            load(n + DS)

    def product_x(n, here=False):
        if not here:
            loaded(n)
        with jax.named_scope("dot2"):
            p = jnp.dot(h[others], dn[n % DS], preferred_element_type=F32)
            xkeep[n] = p[:, :HC]
            xpart[n] = p[:, HC:].astype(BF16)
        swap_x(n).start()

    def product_o(n):
        with jax.named_scope("dot2"):
            p = jnp.dot(h[own], dn[n % DS], preferred_element_type=F32)
            okeep[n] = p[:, :HC]
            opart[n] = p[:, HC:].astype(BF16)
        swap_o(n).start()
        more(n)

    def products(n, m):
        loaded(n)
        with jax.named_scope("dot2b"):
            p = jnp.dot(h[others], dn[n % DS], preferred_element_type=F32)
            r = jnp.dot(h[own], dn[m % DS], preferred_element_type=F32)
            xkeep[n] = p[:, :HC]
            xpart[n] = p[:, HC:].astype(BF16)
            okeep[m] = r[:, :HC]
            opart[m] = r[:, HC:].astype(BF16)
        swap_x(n).start()
        swap_o(m).start()
        more(m)

    def last_products(m):
        loaded(NN - 1)
        p = jnp.dot(h[others], dn[(NN - 1) % DS], preferred_element_type=F32)
        r = jnp.dot(h[own], dn[m % DS], preferred_element_type=F32)
        for i in range(2):
            xkeep[NN - 1 + i] = p[:, i * HC:(i + 1) * HC]
            xpart[NN - 1 + i] = p[:, i * HC:(i + 1) * HC].astype(BF16)
        okeep[m] = r[:, :HC]
        opart[m] = r[:, HC:].astype(BF16)
        swap_o(m).start()

        @pl.when(c == 0)
        def _():
            swap_x(NN - 1).start()
            swap_x(NN).start()

    def last_own_products(m):
        r = jnp.dot(h[own], dn[m % DS], preferred_element_type=F32)
        p = jnp.dot(h[own], dn[(NN - 1) % DS], preferred_element_type=F32)
        okeep[m] = r[:, :HC]
        opart[m] = r[:, HC:].astype(BF16)
        for i in range(2):
            okeep[NN - 1 + i] = p[:, i * HC:(i + 1) * HC]
            opart[NN - 1 + i] = p[:, i * HC:(i + 1) * HC].astype(BF16)
        swap_o(m).start()

        @pl.when(c == 0)
        def _():
            swap_o(NN - 1).start()
            swap_o(NN).start()

    def pass_y(n):
        with jax.named_scope("wswap"):
            swap_x(n).wait_recv()
        ysend[n] = (xkeep[n] + xgot[n].astype(F32)).astype(BF16)
        cross_y(n, 0).start()
        cross_y(n, 1).start()

    def pass_x(n, q):
        if q == 0:
            with jax.named_scope("wswapo"):
                swap_o(n).wait_recv()
        with jax.named_scope("wy"):
            cross_y(n, q).wait_recv()
        r = part(q)
        xsend[n, r] = (okeep[n, r] + ogot[n, r].astype(F32) + yrecv[n, r].astype(F32)).astype(BF16)
        cross_x(n, q).start()

    def finish(n):
        with jax.named_scope("wx"):
            cross_x(n, 0).wait_recv()
            cross_x(n, 1).wait_recv()
        o[:, columns(n)] = (xsend[n].astype(F32) + xrecv[n].astype(F32)).astype(BF16)
        give(n).start()

    O(0)
    O(1)
    direct(0)
    multiply_part(0, others, c)
    O(2)
    direct(1)
    complete(0)
    multiply_part(0, others, 1 - c)
    free(0)
    O(3)
    direct(2)
    X(1)
    free(1)
    relayed(0)
    X(2)
    free(2)
    direct(3)
    X(3)
    free(3)
    relayed(1)
    direct(4)
    O(4)
    X(4)
    relayed(2)
    F(5)
    relayed(3)
    F(6)
    load(0)
    load(1)
    relayed(4)
    load(2)
    complete(7)
    complete(8)
    arrived(7)
    arrived(8)
    multiply(7, others)
    multiply(8, others)
    load(3)
    complete(9)
    arrived(9)
    last(9, others)
    for n in range(4, DS):
        load(n)
    product_x(0)
    product_x(1)
    loaded(2)
    multiply(7, own)
    product_x(2, True)
    pass_y(0)
    pass_y(1)
    multiply(8, own)
    last(9, own)
    product_o(0)
    pass_y(2)
    products(3, 1)

    @pl.loop(LAG_Y, NN - 2)
    def _(n):
        pass_x(n - LAG_Y, 0)
        products(n + 1, n - 1)
        pass_y(n)
        pass_x(n - LAG_Y, 1)

        @pl.when(n >= LAG_X)
        def _():
            finish(n - LAG_X)

    pass_x(NN - 5, 0)
    last_products(NN - 3)
    pass_y(NN - 2)
    pass_x(NN - 5, 1)
    finish(NN - 8)
    pass_x(NN - 4, 0)
    last_own_products(NN - 2)
    pass_x(NN - 4, 1)

    @pl.when(c == 1)
    def _():
        pass_y(NN - 1)
        pass_y(NN)

    finish(NN - 7)
    for n in (NN - 3, NN - 2):
        pass_x(n, 0)
        pass_x(n, 1)
        finish(n - 3)

    @pl.when(c == 1)
    def _():
        for n in (NN - 1, NN):
            pass_x(n, 0)
            pass_x(n, 1)

    for n in (NN - 4, NN - 3, NN - 2):
        finish(n)

    @pl.when(c == 1)
    def _():
        finish(NN - 1)
        finish(NN)

    for core in range(2):
        mine, gone = (NN - 1, NB) if core == 0 else (NB, NN - 1)

        @pl.when(c == core)
        def _():
            with jax.named_scope("wgive"):
                theirs = xpart.at[pl.ds(0, gone)]
                pltpu.make_async_copy(theirs, theirs, out_o.at[0]).wait()
            all_sent(20 + 2 * gone + 3 * mine)


def solution(mesh):
    dma = pltpu.SemaphoreType.DMA
    vmem = pltpu.VMEM

    def step(x, w_gate, w_up, w_down):
        return pl.pallas_call(
            kernel,
            out_shape=pltpu.VMEM((ROWS, D), BF16),
            in_specs=[pl.BlockSpec(memory_space=pl.ANY)] * 4,
            out_specs=pl.BlockSpec(memory_space=pltpu.VMEM),
            scratch_shapes=[
                vmem((NK, 2 * ROWS, KC), BF16),
                vmem((2 * ROWS, 2 * U), F32),
                vmem((2 * ROWS, U), BF16),
                vmem((GS, 2, KC, U), BF16),
                vmem((DS, U, NC), BF16),
                *[vmem((NB, ROWS, HC), F32)] * 2,
                *[vmem((NB, ROWS, HC), BF16)] * 8,
                dma((1,)),
                dma((GS,)),
                dma((DS,)),
                dma((5,)),
                dma((5,)),
                dma((10,)),
                *[dma((RING,))] * 2,
                dma((2 * RING_Y,)),
                dma((2 * RING_X,)),
                dma((1,)),
                dma((1,)),
            ],
            compiler_params=pltpu.CompilerParams(
                collective_id=0, has_side_effects=True, vmem_limit_bytes=61 * 2**20),
        )(x, w_gate, w_up, w_down)

    return jax.shard_map(
        step,
        mesh=mesh,
        in_specs=(P("dp", None), P(None, "tp"), P(None, "tp"), P("tp", None)),
        out_specs=P("dp", None),
        check_vma=False,
    )
```

```python
import jax
import jax.numpy as jnp
from jax import lax
from jax.experimental import pallas as pl
from jax.experimental.pallas import tpu as pltpu
from jax.sharding import PartitionSpec as P

MESH = pl.DeviceIdType.MESH
ROWS, D, FF = 128, 5120, 4480
U = 2304
SKIP = FF - U
KC = 512
NK = D // KC
NC = 512
NN = D // NC
HC = NC // 2
NB = NN + 1
GS = 6
DS = 5
LAG_Y, LAG_X = 3, 6
RING, RING_Y, RING_X = 6, 8, 9
F32, BF16 = jnp.float32, jnp.bfloat16


def kernel(x, wg, wu, wd, o, xs, acc, h, gu, dn, xkeep, okeep, xpart, xgot, opart, ogot, ysend, yrecv, xsend, xrecv,
           xsem, gsem, dsem, in_y, in_x, in_m, sx, so, out_y, out_x, out_o, sent):
    d, t = lax.axis_index("dp"), lax.axis_index("tp")
    xi, c = t // 2, t % 2
    mate, ypeer, xpeer = (d, t + 1 - 2 * c), (1 - d, t), (d, (t + 2) % 4)
    unit0 = pl.multiple_of(d * SKIP, 128)

    def remote(src, dst, sems, i, peer):
        return pltpu.make_async_remote_copy(
            src_ref=src, dst_ref=dst, send_sem=sent.at[0], recv_sem=sems.at[i],
            device_id=peer, device_id_type=MESH)

    def all_sent(blocks):
        some = dn.at[pl.ds(0, 2), pl.ds(0, blocks * ROWS * HC // (2 * NC))]
        pltpu.make_async_copy(some, some, sent.at[0]).wait()

    def chunk(i):
        pair = (i - 2) // 2
        j = jnp.where(i < 2, i, jnp.where(i < 8, jnp.where(i % 2 == 0, pair + 2, pair), i - 5))
        relayed = jnp.where(i < 8, jnp.where(i < 2, 0, i % 2), 1)
        return 2 * j + jnp.where(relayed == 1, 1 - xi, xi)

    def x_own(k):
        return pltpu.make_async_copy(x.at[:, pl.ds(k * KC, KC)], xs.at[k, pl.ds(0, ROWS)], xsem.at[0])

    def slab(i, which):
        w = (wg, wu)[which]
        rows = pl.ds(pl.multiple_of(chunk(i) * KC, KC), KC)
        s = i % GS
        return pltpu.make_async_copy(w.at[rows, pl.ds(unit0, U)], gu.at[s, which], gsem.at[s])

    def down(n, half):
        s = n % DS
        first = jnp.where(n == NN - 1, half, jnp.where(half == 0, c, 1 - c))
        cols = pl.ds(pl.multiple_of(n * NC + first * HC, HC), HC)
        return pltpu.make_async_copy(
            wd.at[pl.ds(unit0, U), cols], dn.at[s, :, pl.ds(half * HC, HC)], dsem.at[s])

    def load(n):
        down(n, 0).start(priority=1)
        down(n, 1).start(priority=1)

    def other(k, core):
        return xs.at[k, pl.ds(ROWS, ROWS), pl.ds(pl.multiple_of(core * (KC // 2), KC // 2), KC // 2)]

    def mine_x(k):
        return xs.at[k, pl.ds(0, ROWS), pl.ds(pl.multiple_of(c * (KC // 2), KC // 2), KC // 2)]

    def send_y(j):
        return remote(mine_x(2 * j + xi), other(2 * j + xi, c), in_y, j, ypeer)

    def relay_x(j):
        return remote(other(2 * j + xi, c), other(2 * j + xi, c), in_x, j, xpeer)

    def got_x(j):
        return remote(other(2 * j + 1 - xi, c), other(2 * j + 1 - xi, c), in_x, j, xpeer)

    def to_mate(j, relayed):
        k = 2 * j + (1 - xi if relayed else xi)
        return remote(other(k, c), other(k, c), in_m, j + 5 * relayed, mate)

    def from_mate(j, relayed):
        k = 2 * j + (1 - xi if relayed else xi)
        return remote(other(k, 1 - c), other(k, 1 - c), in_m, j + 5 * relayed, mate)

    barrier = pltpu.get_barrier_semaphore()
    for peer in (mate, ypeer, xpeer):
        pl.semaphore_signal(barrier, inc=1, device_id=peer, device_id_type=MESH)
    for k in range(NK):
        x_own(k).start()
    for i in range(GS):
        slab(i, 0).start(priority=1)
        slab(i, 1).start(priority=1)
    acc[...] = jnp.zeros_like(acc)
    with jax.named_scope("bar"):
        pl.semaphore_wait(barrier, 3)
    with jax.named_scope("wxown"):
        pltpu.make_async_copy(x, o, xsem.at[0]).wait()
    for j in range(5):
        send_y(j).start()
    def direct(j):
        with jax.named_scope("wdirect"):
            send_y(j).wait_recv()
        relay_x(j).start()
        to_mate(j, 0).start()

    def relayed(j):
        with jax.named_scope("wrelay"):
            got_x(j).wait_recv()
        to_mate(j, 1).start()

    def whole(j, was_relayed):
        with jax.named_scope("wmate"):
            from_mate(j, was_relayed).wait_recv()

    here = set()

    def arrived(i):
        if i in here:
            return
        here.add(i)
        with jax.named_scope("wslab"):
            pltpu.make_async_copy(gu.at[i % GS], gu.at[i % GS], gsem.at[i % GS]).wait()

    def free(i):
        if i + GS < NK:
            slab(i + GS, 0).start(priority=1)
            slab(i + GS, 1).start(priority=1)

    def multiply(i, rows):
        xk = xs[chunk(i), rows]
        with jax.named_scope("dot1"):
            for which in range(2):
                acc[rows, which * U:(which + 1) * U] += jnp.dot(xk, gu[i % GS, which], preferred_element_type=F32)

    own, others, both = slice(0, ROWS), slice(ROWS, 2 * ROWS), slice(0, 2 * ROWS)
    relayed_ones = {3: 0, 5: 1, 7: 2, 8: 3, 9: 4}
    direct_ones = {0: 0, 1: 1, 2: 2, 4: 3, 6: 4}

    def complete(i):
        if i in relayed_ones:
            whole(relayed_ones[i], 1)
        else:
            whole(direct_ones[i], 0)

    def multiply_part(i, rows, core):
        cut = pl.ds(pl.multiple_of(core * (KC // 2), KC // 2), KC // 2)
        xk = xs[chunk(i), rows, cut]
        with jax.named_scope("dot1p"):
            for which in range(2):
                acc[rows, which * U:(which + 1) * U] += jnp.dot(
                    xk, gu[i % GS, which, cut], preferred_element_type=F32)

    def last(i, rows):
        xk = xs[chunk(i), rows]
        with jax.named_scope("dot1last"):
            for b in range(U // 256):
                gate, up = (
                    acc[rows, w * U + b * 256:w * U + (b + 1) * 256]
                    + jnp.dot(xk, gu[i % GS, w, :, b * 256:(b + 1) * 256], preferred_element_type=F32)
                    for w in range(2))
                h[rows, b * 256:(b + 1) * 256] = (jax.nn.silu(gate) * up).astype(BF16)

        @pl.when(d == 1)
        def _():
            h[rows, 0:2 * U - FF] = jnp.zeros((ROWS, 2 * U - FF), BF16)

    def O(*steps):
        for i in steps:
            arrived(i)
        for i in steps:
            multiply(i, own)

    def X(*steps):
        for i in steps:
            complete(i)
        for i in steps:
            arrived(i)
        for i in steps:
            multiply(i, others)

    def F(*steps):
        for i in steps:
            complete(i)
        for i in steps:
            arrived(i)
        for i in steps:
            multiply(i, both)

    def swap_x(n):
        return remote(xpart.at[n], xgot.at[n], sx, n % RING, mate)

    def swap_o(n):
        return remote(opart.at[n], ogot.at[n], so, n % RING, mate)

    def part(q):
        return pl.ds(q * (ROWS // 2), ROWS // 2)

    def cross_y(n, q):
        return remote(ysend.at[n, part(q)], yrecv.at[n, part(q)], out_y, 2 * (n % RING_Y) + q, ypeer)

    def cross_x(n, q):
        return remote(xsend.at[n, part(q)], xrecv.at[n, part(q)], out_x, 2 * (n % RING_X) + q, xpeer)

    def columns(n):
        start = jnp.where(n < NN - 1, n * NC + c * HC, (NN - 1) * NC + (n - NN + 1) * HC)
        return pl.ds(pl.multiple_of(start, HC), HC)

    def give(n):
        return remote(o.at[:, columns(n)], o.at[:, columns(n)], out_o, 0, mate)

    def loaded(n):
        with jax.named_scope("wdown"):
            pltpu.make_async_copy(dn.at[n % DS], dn.at[n % DS], dsem.at[n % DS]).wait()

    def more(n):
        @pl.when(n + DS < NN)
        def _():
            load(n + DS)

    def product_x(n, here=False):
        if not here:
            loaded(n)
        with jax.named_scope("dot2"):
            p = jnp.dot(h[others], dn[n % DS], preferred_element_type=F32)
            xkeep[n] = p[:, :HC]
            xpart[n] = p[:, HC:].astype(BF16)
        swap_x(n).start()

    def product_o(n):
        with jax.named_scope("dot2"):
            p = jnp.dot(h[own], dn[n % DS], preferred_element_type=F32)
            okeep[n] = p[:, :HC]
            opart[n] = p[:, HC:].astype(BF16)
        swap_o(n).start()
        more(n)

    def products(n, m):
        loaded(n)
        with jax.named_scope("dot2b"):
            p = jnp.dot(h[others], dn[n % DS], preferred_element_type=F32)
            r = jnp.dot(h[own], dn[m % DS], preferred_element_type=F32)
            xkeep[n] = p[:, :HC]
            xpart[n] = p[:, HC:].astype(BF16)
            okeep[m] = r[:, :HC]
            opart[m] = r[:, HC:].astype(BF16)
        swap_x(n).start()
        swap_o(m).start()
        more(m)

    def last_products(m):
        loaded(NN - 1)
        p = jnp.dot(h[others], dn[(NN - 1) % DS], preferred_element_type=F32)
        r = jnp.dot(h[own], dn[m % DS], preferred_element_type=F32)
        for i in range(2):
            xkeep[NN - 1 + i] = p[:, i * HC:(i + 1) * HC]
            xpart[NN - 1 + i] = p[:, i * HC:(i + 1) * HC].astype(BF16)
        okeep[m] = r[:, :HC]
        opart[m] = r[:, HC:].astype(BF16)

        @pl.when(c == 0)
        def _():
            swap_x(NN - 1).start()
            swap_x(NN).start()

        swap_o(m).start()

    def last_own_products(m):
        r = jnp.dot(h[own], dn[m % DS], preferred_element_type=F32)
        p = jnp.dot(h[own], dn[(NN - 1) % DS], preferred_element_type=F32)
        okeep[m] = r[:, :HC]
        opart[m] = r[:, HC:].astype(BF16)
        for i in range(2):
            okeep[NN - 1 + i] = p[:, i * HC:(i + 1) * HC]
            opart[NN - 1 + i] = p[:, i * HC:(i + 1) * HC].astype(BF16)
        swap_o(m).start()

        @pl.when(c == 0)
        def _():
            swap_o(NN - 1).start()
            swap_o(NN).start()

    def pass_y(n):
        with jax.named_scope("wswap"):
            swap_x(n).wait_recv()
        ysend[n] = (xkeep[n] + xgot[n].astype(F32)).astype(BF16)
        cross_y(n, 0).start()
        cross_y(n, 1).start()

    def pass_x(n, q):
        if q == 0:
            with jax.named_scope("wswapo"):
                swap_o(n).wait_recv()
        with jax.named_scope("wy"):
            cross_y(n, q).wait_recv()
        r = part(q)
        xsend[n, r] = (okeep[n, r] + ogot[n, r].astype(F32) + yrecv[n, r].astype(F32)).astype(BF16)
        cross_x(n, q).start()

    def finish(n):
        with jax.named_scope("wx"):
            cross_x(n, 0).wait_recv()
            cross_x(n, 1).wait_recv()
        o[:, columns(n)] = (xsend[n].astype(F32) + xrecv[n].astype(F32)).astype(BF16)
        give(n).start()

    O(0)
    O(1)
    direct(0)
    multiply_part(0, others, c)
    O(2)
    direct(1)
    complete(0)
    multiply_part(0, others, 1 - c)
    free(0)
    O(3)
    direct(2)
    X(1)
    free(1)
    relayed(0)
    X(2)
    free(2)
    direct(3)
    X(3)
    free(3)
    relayed(1)
    direct(4)
    O(4)
    X(4)
    relayed(2)
    F(5)
    relayed(3)
    F(6)
    load(0)
    load(1)
    relayed(4)
    load(2)
    complete(7)
    complete(8)
    arrived(7)
    arrived(8)
    multiply(7, others)
    multiply(8, others)
    load(3)
    complete(9)
    arrived(9)
    last(9, others)
    for n in range(4, DS):
        load(n)
    product_x(0)
    product_x(1)
    loaded(2)
    multiply(7, own)
    product_x(2, True)
    pass_y(0)
    pass_y(1)
    multiply(8, own)
    last(9, own)
    product_o(0)
    pass_y(2)
    products(3, 1)

    @pl.loop(LAG_Y, NN - 2)
    def _(n):
        pass_x(n - LAG_Y, 0)
        products(n + 1, n - 1)
        pass_y(n)
        pass_x(n - LAG_Y, 1)

        @pl.when(n >= LAG_X)
        def _():
            finish(n - LAG_X)

    pass_x(NN - 5, 0)
    last_products(NN - 3)
    pass_y(NN - 2)
    pass_x(NN - 5, 1)
    finish(NN - 8)
    pass_x(NN - 4, 0)
    last_own_products(NN - 2)
    pass_x(NN - 4, 1)

    @pl.when(c == 1)
    def _():
        pass_y(NN - 1)
        pass_y(NN)

    finish(NN - 7)
    for n in (NN - 3, NN - 2):
        pass_x(n, 0)
        pass_x(n, 1)
        finish(n - 3)

    @pl.when(c == 1)
    def _():
        for n in (NN - 1, NN):
            pass_x(n, 0)
            pass_x(n, 1)

    for n in (NN - 4, NN - 3, NN - 2):
        finish(n)

    @pl.when(c == 1)
    def _():
        finish(NN - 1)
        finish(NN)

    for core in range(2):
        mine, gone = (NN - 1, NB) if core == 0 else (NB, NN - 1)

        @pl.when(c == core)
        def _():
            with jax.named_scope("wgive"):
                theirs = xpart.at[pl.ds(0, gone)]
                pltpu.make_async_copy(theirs, theirs, out_o.at[0]).wait()
            all_sent(20 + 2 * gone + 3 * mine)


def solution(mesh):
    dma = pltpu.SemaphoreType.DMA
    vmem = pltpu.VMEM

    def step(x, w_gate, w_up, w_down):
        return pl.pallas_call(
            kernel,
            out_shape=pltpu.VMEM((ROWS, D), BF16),
            in_specs=[pl.BlockSpec(memory_space=pl.ANY)] * 4,
            out_specs=pl.BlockSpec(memory_space=pltpu.VMEM),
            scratch_shapes=[
                vmem((NK, 2 * ROWS, KC), BF16),
                vmem((2 * ROWS, 2 * U), F32),
                vmem((2 * ROWS, U), BF16),
                vmem((GS, 2, KC, U), BF16),
                vmem((DS, U, NC), BF16),
                *[vmem((NB, ROWS, HC), F32)] * 2,
                *[vmem((NB, ROWS, HC), BF16)] * 8,
                dma((1,)),
                dma((GS,)),
                dma((DS,)),
                dma((5,)),
                dma((5,)),
                dma((10,)),
                *[dma((RING,))] * 2,
                dma((2 * RING_Y,)),
                dma((2 * RING_X,)),
                dma((1,)),
                dma((1,)),
            ],
            compiler_params=pltpu.CompilerParams(
                collective_id=0, has_side_effects=True, vmem_limit_bytes=61 * 2**20),
        )(x, w_gate, w_up, w_down)

    return jax.shard_map(
        step,
        mesh=mesh,
        in_specs=(P("dp", None), P(None, "tp"), P(None, "tp"), P("tp", None)),
        out_specs=P("dp", None),
        check_vma=False,
    )
```
